128 devices in a mesh: dp: 2 (over core), emb: 64 (over z, y, x).
Axes of the slice: x: 4, y: 4, z: 4, core: 2. Of those that a mesh axis runs over, the one named last changes fastest.
Arguments:
- tok_ids: int32 [32768], P(('dp', 'emb'))
- resid_in: bfloat16 [32768, 1152], P(('dp', 'emb'))
- cot_out: bfloat16 [32768, 1152], P(('dp', 'emb'))
- tables: bfloat16 [3, 262144, 256], P(None, 'emb')
- w_up: bfloat16 [3, 1152, 6912], replicated
- w_down: bfloat16 [3, 6912, 1152], replicated
- w_gate: bfloat16 [3, 1152, 256], replicated
- w_proj: bfloat16 [3, 256, 1152], replicated
Outputs:
- output 1: bfloat16 [32768, 1152], P(('dp', 'emb'))
- output 2: float32 [3, 262144, 256], P(None, 'emb')
All inputs are finite; a program needn't handle non-finite values.
Results may differ from the reference program's by a relative error of at most 0.012038.
Values are sent between devices in bfloat16 or wider.
A program may use at most 1 GiB of HBM per device.

```python
import jax
import jax.numpy as jnp
from jax import lax

TOKENS_DEV = 256
LAYERS = 3
D_MODEL = 1152
FFN_DIM = 6912
EMB_DIM = 256
VOCAB_SIZE = 262144
NUM_DP = 2
NUM_EMB = 64
CAP_ROWS = 8

N_TOKENS = TOKENS_DEV * NUM_DP * NUM_EMB
RANGE_ROWS = VOCAB_SIZE // NUM_EMB
HOT_SET = min(16, RANGE_ROWS)
NORM_EPS = 1e-6


def draw_ids(id_key):
    key_list = jax.random.split(id_key, 9)
    n_dev = NUM_DP * NUM_EMB
    draw_shape = (n_dev, TOKENS_DEV)
    tok_pos = jnp.arange(TOKENS_DEV, dtype=jnp.int32)[None, :]
    hot_top = jax.random.randint(key_list[0], (n_dev, 1), 1, NUM_EMB + 1)
    hot_owner = jax.random.randint(key_list[1], (n_dev, 1), 0, hot_top)
    shift_by = jax.random.randint(key_list[2], (n_dev, 1), 0, NUM_EMB - 1)
    spread = (hot_owner + 1 + (tok_pos - CAP_ROWS + shift_by) % (NUM_EMB - 1)) % NUM_EMB
    owner_seq = jnp.where(tok_pos < CAP_ROWS, hot_owner, spread)
    scores = jax.random.randint(key_list[3], draw_shape, 0, TOKENS_DEV) * TOKENS_DEV + tok_pos
    perm_order = jnp.argsort(scores, axis=1)
    owner_ids = jnp.take_along_axis(owner_seq, perm_order, axis=1)
    is_hot = jax.random.randint(key_list[4], draw_shape, 0, 4) == 0
    hot_off = jax.random.randint(key_list[5], draw_shape, 0, HOT_SET)
    span_a = jax.random.randint(key_list[6], draw_shape, 1, RANGE_ROWS + 1)
    span_b = jax.random.randint(key_list[7], draw_shape, 1, span_a + 1)
    tail_off = jax.random.randint(key_list[8], draw_shape, 0, span_b)
    offset = jnp.where(is_hot, hot_off, tail_off)
    return (owner_ids * RANGE_ROWS + offset).reshape(-1).astype(jnp.int32)


def setup_inputs(seed: int = 0) -> dict:
    root_key = jax.random.key(seed)
    key_list = jax.random.split(root_key, 8)
    tok_ids = draw_ids(key_list[0])
    resid_in = jax.random.normal(key_list[1], (N_TOKENS, D_MODEL), jnp.float32).astype(jnp.bfloat16)
    cot_out = jax.random.normal(key_list[2], (N_TOKENS, D_MODEL), jnp.float32).astype(jnp.bfloat16)
    tables = (0.5 * jax.random.normal(key_list[3], (LAYERS, VOCAB_SIZE, EMB_DIM), jnp.float32)).astype(jnp.bfloat16)
    w_up = (jax.random.normal(key_list[4], (LAYERS, D_MODEL, FFN_DIM), jnp.float32) * D_MODEL ** -0.5).astype(jnp.bfloat16)
    w_down = (jax.random.normal(key_list[5], (LAYERS, FFN_DIM, D_MODEL), jnp.float32) * (0.5 * FFN_DIM ** -0.5)).astype(jnp.bfloat16)
    w_gate = (jax.random.normal(key_list[6], (LAYERS, D_MODEL, EMB_DIM), jnp.float32) * D_MODEL ** -0.5).astype(jnp.bfloat16)
    w_proj = (jax.random.normal(key_list[7], (LAYERS, EMB_DIM, D_MODEL), jnp.float32) * EMB_DIM ** -0.5).astype(jnp.bfloat16)
    return {'tok_ids': tok_ids, 'resid_in': resid_in, 'cot_out': cot_out, 'tables': tables, 'w_up': w_up, 'w_down': w_down, 'w_gate': w_gate, 'w_proj': w_proj}


def rms_norm(x_f32):
    return x_f32 * lax.rsqrt(jnp.mean(x_f32 * x_f32, axis=-1, keepdims=True) + NORM_EPS)


def layer_forward(resid_cur, fetched, w_up_l, w_down_l, w_gate_l, w_proj_l):
    x_f32 = resid_cur.astype(jnp.float32)
    normed = rms_norm(x_f32).astype(jnp.bfloat16)
    hidden = jax.nn.gelu(jnp.dot(normed, w_up_l, preferred_element_type=jnp.float32)).astype(jnp.bfloat16)
    mlp_out = jnp.dot(hidden, w_down_l, preferred_element_type=jnp.float32)
    gate_act = jax.nn.gelu(jnp.dot(normed, w_gate_l, preferred_element_type=jnp.float32))
    mixed_in = (gate_act * fetched).astype(jnp.bfloat16)
    proj_out = jnp.dot(mixed_in, w_proj_l, preferred_element_type=jnp.float32)
    return (x_f32 + mlp_out + proj_out).astype(jnp.bfloat16)


def reference(tok_ids, resid_in, cot_out, tables, w_up, w_down, w_gate, w_proj):
    def fwd_step(resid_cur, layer_params):
        table_l, w_up_l, w_down_l, w_gate_l, w_proj_l = layer_params
        fetched = jnp.take(table_l, tok_ids, axis=0).astype(jnp.float32)
        resid_next = layer_forward(resid_cur, fetched, w_up_l, w_down_l, w_gate_l, w_proj_l)
        return resid_next, resid_cur

    resid_out, resid_saved = lax.scan(fwd_step, resid_in, (tables, w_up, w_down, w_gate, w_proj))

    def bwd_step(cot_next, layer_params):
        resid_cur, table_l, w_up_l, w_down_l, w_gate_l, w_proj_l = layer_params
        fetched = jnp.take(table_l, tok_ids, axis=0).astype(jnp.float32)

        def local_layer(resid_arg, fetched_arg):
            return layer_forward(resid_arg, fetched_arg, w_up_l, w_down_l, w_gate_l, w_proj_l)

        pullback = jax.vjp(local_layer, resid_cur, fetched)[1]
        cot_cur, d_fetched = pullback(cot_next)
        d_table = jax.ops.segment_sum(d_fetched, tok_ids, num_segments=VOCAB_SIZE)
        return cot_cur, d_table

    cot_first, d_tables = lax.scan(bwd_step, cot_out, (resid_saved, tables, w_up, w_down, w_gate, w_proj), reverse=True)
    return resid_out, d_tables
```

```python
import functools
import math

import jax
import jax.numpy as jnp
from jax import lax
from jax.experimental import pallas as pl
from jax.experimental.pallas import tpu as pltpu
from jax.sharding import PartitionSpec as P

NORM_EPS = 1e-6
CAP = 8
BF = jnp.bfloat16
F32 = jnp.float32
MESH_ID = pl.DeviceIdType.MESH
VMEM_LIMIT = 60 * 1024 * 1024
GELU_C = math.sqrt(2.0 / math.pi)


def dot(a, b):
    return jnp.dot(a, b, preferred_element_type=F32)


def dot_nt(a, b):
    return lax.dot_general(a, b, (((1,), (1,)), ((), ())), preferred_element_type=F32)


def dot_tn(a, b):
    return lax.dot_general(a, b, (((0,), (0,)), ((), ())), preferred_element_type=F32)


def iota(shape, axis):
    return lax.broadcasted_iota(jnp.int32, shape, axis)


def gelu_both(x):
    x2 = x * x
    t = jnp.tanh(x * (GELU_C + (GELU_C * 0.044715) * x2))
    hx = 0.5 * x
    s = 0.5 + 0.5 * t
    d = s + hx * (1.0 - t * t) * (GELU_C + (3.0 * GELU_C * 0.044715) * x2)
    return x * s, d


def inv_rms(x):
    return lax.rsqrt(jnp.mean(x * x, axis=-1, keepdims=True) + NORM_EPS)


def peers_barrier(n_emb):
    me, dp = lax.axis_index("emb"), lax.axis_index("dp")
    bar = pltpu.get_barrier_semaphore()

    def tell(k, carry):
        pl.semaphore_signal(bar, inc=1, device_id={"emb": lax.rem(me + k, n_emb)}, device_id_type=MESH_ID)
        return carry

    lax.fori_loop(1, n_emb, tell, 0)
    pl.semaphore_signal(bar, inc=1, device_id={"dp": 1 - dp}, device_id_type=MESH_ID)
    return bar


def send_blocks(n_emb, src, dst, send_sem, recv_sem):
    me = lax.axis_index("emb")

    def one(k, carry):
        to = lax.rem(me + k, n_emb)
        pltpu.make_async_remote_copy(
            src_ref=src.at[to], dst_ref=dst.at[me], send_sem=send_sem, recv_sem=recv_sem,
            device_id={"emb": to}, device_id_type=MESH_ID).start()
        return carry

    lax.fori_loop(1, n_emb, one, 0)


def blocks_desc(n_emb, src, dst, send_sem, recv_sem):
    me = lax.axis_index("emb")
    return pltpu.make_async_remote_copy(
        src_ref=src.at[pl.ds(0, n_emb - 1)], dst_ref=dst.at[pl.ds(0, n_emb - 1)],
        send_sem=send_sem, recv_sem=recv_sem, device_id={"emb": me}, device_id_type=MESH_ID)


def partner_copy(src, dst, send_sem, recv_sem):
    return pltpu.make_async_remote_copy(
        src_ref=src, dst_ref=dst, send_sem=send_sem, recv_sem=recv_sem,
        device_id={"dp": 1 - lax.axis_index("dp")}, device_id_type=MESH_ID)


def fetch_kernel(n_emb, ids_ref, table_hbm, fetched_ref, st_ref, rid_ref,
                 table, sid, rows_out, rows_in, acc, tsem, isem, rsem, psem):
    me = lax.axis_index("emb")
    n_layers, n_rows, e = table.shape
    t = ids_ref.shape[1]
    n_slots = n_emb * CAP
    shift = n_rows.bit_length() - 1
    loads = [pltpu.make_async_copy(table_hbm.at[l], table.at[l], tsem.at[l]) for l in range(n_layers)]
    for ld in loads:
        ld.start()
    bar = peers_barrier(n_emb)

    ids = ids_ref[...]
    owner = lax.shift_right_logical(ids, shift)
    local = ids - lax.shift_left(owner, shift) + 1
    own_t = owner == iota((n_emb, t), 0)
    before = (iota((t, t), 0) < iota((t, t), 1)).astype(F32).astype(BF)
    own_f = own_t.astype(F32)
    rank = jnp.sum(own_f * dot(own_f.astype(BF), before), axis=0, keepdims=True).astype(jnp.int32)
    slot = owner * CAP + rank
    st = (slot == iota((n_slots, t), 0)).astype(F32).astype(BF)
    st_ref[...] = st
    rank_t = (rank == iota((128, t), 0)).astype(F32).astype(BF)
    hi = jnp.where(own_t, lax.shift_right_logical(local, 6).astype(F32), 0.0).astype(BF)
    lo = jnp.where(own_t, jnp.bitwise_and(local, 63).astype(F32), 0.0).astype(BF)
    sid[...] = (64.0 * dot_nt(hi, rank_t) + dot_nt(lo, rank_t)).astype(jnp.int32).reshape(sid.shape)

    pl.semaphore_wait(bar, n_emb)
    mine = rid_ref.at[0]
    send_blocks(n_emb, sid, mine, isem.at[0], isem.at[1])
    rid_ref[0, me] = sid[me]
    got = blocks_desc(n_emb, sid, mine, isem.at[0], isem.at[1])
    got.wait()
    to_partner = partner_copy(mine, rid_ref.at[1], psem.at[0], psem.at[1])
    to_partner.start()

    ids_in = rid_ref[0].reshape(n_emb, 128)
    spread = (lax.shift_right_logical(iota((n_slots, n_emb), 0), 3) == iota((n_slots, n_emb), 1)).astype(F32).astype(BF)
    hi = lax.shift_right_logical(ids_in, 6).astype(F32).astype(BF)
    lo = jnp.bitwise_and(ids_in, 63).astype(F32).astype(BF)
    wide = 64.0 * dot(spread, hi) + dot(spread, lo)
    pick = jnp.bitwise_and(iota((n_slots, 128), 0), CAP - 1) == iota((n_slots, 128), 1)
    col = (jnp.sum(jnp.where(pick, wide, 0.0), axis=1, keepdims=True)).astype(jnp.int32) - 1
    for ld in loads:
        ld.wait()
    step = min(1024, n_rows)
    for c in range(n_rows // step):
        oh = (col == iota((n_slots, step), 1) + c * step).astype(F32).astype(BF)
        for l in range(n_layers):
            part = dot(oh, table[l, c * step:(c + 1) * step, :])
            if c == 0:
                acc[l] = part
            else:
                acc[l] += part
    for l in range(n_layers):
        rows_out[l] = acc[l].astype(BF).reshape(n_emb, CAP, e)
        send_blocks(n_emb, rows_out.at[l], rows_in.at[l], rsem.at[0, l], rsem.at[1, l])
        rows_in[l, me] = rows_out[l, me]
    for l in range(n_layers):
        blocks_desc(n_emb, rows_out.at[l], rows_in.at[l], rsem.at[0, l], rsem.at[1, l]).wait()
        fetched_ref[l] = dot_tn(st, rows_in[l].reshape(n_slots, e)).astype(BF)
    to_partner.wait()


def fetch(n_emb, tok_ids, tables):
    n_layers, n_rows, e = tables.shape
    t = tok_ids.shape[0]
    n_slots = n_emb * CAP
    vmem = pl.BlockSpec(memory_space=pltpu.VMEM)
    return pl.pallas_call(
        functools.partial(fetch_kernel, n_emb),
        out_shape=(jax.ShapeDtypeStruct((n_layers, t, e), BF),
                   jax.ShapeDtypeStruct((n_slots, t), BF),
                   jax.ShapeDtypeStruct((2, n_emb, 1, 128), jnp.int32)),
        in_specs=[vmem, pl.BlockSpec(memory_space=pl.ANY)],
        out_specs=(vmem, vmem, vmem),
        scratch_shapes=[
            pltpu.VMEM((n_layers, n_rows, e), BF),
            pltpu.VMEM((n_emb, 1, 128), jnp.int32),
            pltpu.VMEM((n_layers, n_emb, CAP, e), BF),
            pltpu.VMEM((n_layers, n_emb, CAP, e), BF),
            pltpu.VMEM((n_layers, n_slots, e), F32),
            pltpu.SemaphoreType.DMA((n_layers,)),
            pltpu.SemaphoreType.DMA((2,)),
            pltpu.SemaphoreType.DMA((2, n_layers)),
            pltpu.SemaphoreType.DMA((2,)),
        ],
        compiler_params=pltpu.CompilerParams(collective_id=0, has_side_effects=True, vmem_limit_bytes=VMEM_LIMIT),
        name="fetch",
    )(tok_ids.reshape(1, t), tables)


RING = 4


def dense_kernel(n_layers, resid_ref, cot_ref, fetched_ref, st_ref, up_hbm, down_hbm, gate_hbm, proj_hbm,
                 out_ref, grad_ref,
                 wup, wdn, gate, proj, gp, acc, xs, us, cots, hid, gval, gder, upsem, dnsem, gsem):
    t, d = resid_ref.shape
    tf = wup.shape[2]
    n_chunks = up_hbm.shape[2] // tf
    n_pass = 2 * n_layers - 1
    total = n_pass * n_chunks

    def layer_of(g):
        p = g // n_chunks
        return jnp.minimum(p, 2 * n_layers - 1 - p)

    def up_copy(g):
        c = lax.rem(g, n_chunks)
        return pltpu.make_async_copy(up_hbm.at[layer_of(g), :, pl.ds(pl.multiple_of(c * tf, tf), tf)],
                                     wup.at[lax.rem(g, RING)], upsem.at[lax.rem(g, RING)])

    def dn_copy(g):
        c = lax.rem(g, n_chunks)
        return pltpu.make_async_copy(down_hbm.at[layer_of(g), pl.ds(pl.multiple_of(c * tf, tf), tf), :],
                                     wdn.at[lax.rem(g, RING)], dnsem.at[lax.rem(g, RING)])

    def start(copy, g):
        @pl.when(g < total)
        def _():
            copy(g).start()

    gate_loads = [pltpu.make_async_copy(gate_hbm, gate, gsem.at[0]), pltpu.make_async_copy(proj_hbm, proj, gsem.at[1])]
    for g in range(RING):
        up_copy(jnp.int32(g)).start()
        dn_copy(jnp.int32(g)).start()
        if g == 0:
            for ld in gate_loads:
                ld.start()

    xs[0] = resid_ref[...]
    for ld in gate_loads:
        ld.wait()

    n_sub = tf // 256

    def fwd_up(l, g, c, hslot):
        up_copy(g).wait()
        w = wup.at[lax.rem(g, RING)]
        for j in range(n_sub):
            cols = slice(j * 256, (j + 1) * 256)
            h, der = gelu_both(dot(us[...], w[:, cols]))
            hid[hslot, :, cols] = h.astype(BF)
            gp[lax.rem(l + 1, 2), c, :, cols] = der
        start(up_copy, g + RING)

    def fwd_down(g, hslot):
        dn_copy(g).wait()
        acc[...] += dot(hid[hslot], wdn[lax.rem(g, RING)])
        start(dn_copy, g + RING)

    def bwd_down(l, g, c, hslot):
        dn_copy(g).wait()
        w = wdn.at[lax.rem(g, RING)]
        for j in range(n_sub):
            cols = slice(j * 256, (j + 1) * 256)
            dh = dot_nt(cots[...], w[cols, :]).astype(BF).astype(F32)
            hid[hslot, :, cols] = (gp[lax.rem(l + 1, 2), c, :, cols] * dh).astype(BF)
        start(dn_copy, g + RING)

    def bwd_up(g, hslot):
        up_copy(g).wait()
        acc[...] += dot_nt(hid[hslot], wup[lax.rem(g, RING)])
        start(up_copy, g + RING)

    def sweep(g0, first, second):
        first(g0, 0, 0)

        def pair(i, carry):
            c = 2 * i
            first(g0 + c + 1, c + 1, 1)
            second(g0 + c, 0)
            first(g0 + c + 2, c + 2, 0)
            second(g0 + c + 1, 1)
            return carry

        lax.fori_loop(0, (n_chunks - 1) // 2, pair, 0)
        second(g0 + n_chunks - 1, 0)

    assert n_chunks % 2 == 1

    def forward(l, carry):
        x = xs[l].astype(F32)
        us[...] = (x * inv_rms(x)).astype(BF)
        g, der = gelu_both(dot(us[...], gate[l]))
        gval[l] = g
        gder[l] = der
        mixed = (g * fetched_ref[l].astype(F32)).astype(BF)
        acc[...] = x + dot(mixed, proj[l])
        sweep(l * n_chunks, functools.partial(fwd_up, l), fwd_down)
        xs[l + 1] = acc[...].astype(BF)
        return carry

    lax.fori_loop(0, n_layers, forward, 0)
    out_ref[...] = xs[n_layers]
    cots[...] = cot_ref[...]

    def table_rows(l):
        d_mixed = dot_nt(cots[...], proj[l]).astype(BF).astype(F32)
        rows = gval[l] * d_mixed
        hi = rows.astype(BF)
        rest = rows - hi.astype(F32)
        mid = rest.astype(BF)
        low = (rest - mid.astype(F32)).astype(BF)
        st = st_ref[...]
        slots = dot(st, hi) + dot(st, mid) + dot(st, low)
        grad_ref[l] = slots.reshape(grad_ref.shape[1:])
        return d_mixed

    def backward(i, carry):
        l = n_layers - 1 - i
        d_mixed = table_rows(l)
        d_gate = (gder[l] * (d_mixed * fetched_ref[l].astype(F32))).astype(BF)
        acc[...] = jnp.zeros_like(acc)
        sweep((n_layers + i) * n_chunks, functools.partial(bwd_down, l), bwd_up)
        d_norm = (acc[...].astype(BF).astype(F32) + dot_nt(d_gate, gate[l]).astype(BF).astype(F32)).astype(BF).astype(F32)
        x = xs[l].astype(F32)
        r = inv_rms(x)
        dx = r * d_norm - x * (r * r * r * jnp.mean(x * d_norm, axis=-1, keepdims=True))
        cots[...] = (cots[...].astype(F32) + dx).astype(BF)
        return carry

    lax.fori_loop(0, n_layers - 1, backward, 0)
    table_rows(0)


def dense(n_emb, resid, cot, fetched, st, w_up, w_down, w_gate, w_proj, tf):
    t, d = resid.shape
    n_layers, _, f = w_up.shape
    e = w_gate.shape[2]
    vmem, hbm = pl.BlockSpec(memory_space=pltpu.VMEM), pl.BlockSpec(memory_space=pl.ANY)
    return pl.pallas_call(
        functools.partial(dense_kernel, n_layers),
        out_shape=(jax.ShapeDtypeStruct((t, d), BF),
                   jax.ShapeDtypeStruct((n_layers, n_emb, CAP, e), F32)),
        in_specs=[vmem] * 4 + [hbm] * 4,
        out_specs=(vmem, vmem),
        scratch_shapes=[
            pltpu.VMEM((RING, d, tf), BF),
            pltpu.VMEM((RING, tf, d), BF),
            pltpu.VMEM((n_layers, d, e), BF),
            pltpu.VMEM((n_layers, e, d), BF),
            pltpu.VMEM((2, f // tf, t, tf), F32),
            pltpu.VMEM((t, d), F32),
            pltpu.VMEM((n_layers + 1, t, d), BF),
            pltpu.VMEM((t, d), BF),
            pltpu.VMEM((t, d), BF),
            pltpu.VMEM((2, t, tf), BF),
            pltpu.VMEM((n_layers, t, e), F32),
            pltpu.VMEM((n_layers, t, e), F32),
            pltpu.SemaphoreType.DMA((RING,)),
            pltpu.SemaphoreType.DMA((RING,)),
            pltpu.SemaphoreType.DMA((2,)),
        ],
        compiler_params=pltpu.CompilerParams(vmem_limit_bytes=VMEM_LIMIT),
        name="dense",
    )(resid, cot, fetched, st, w_up, w_down, w_gate, w_proj)


def return_kernel(n_emb, grad_ref, rows_ref, sem, psem):
    me = lax.axis_index("emb")
    n_layers = grad_ref.shape[0]
    bar = peers_barrier(n_emb)
    pl.semaphore_wait(bar, n_emb)
    order = list(reversed(range(n_layers)))
    for l in order:
        send_blocks(n_emb, grad_ref.at[l], rows_ref.at[0, l], sem.at[0, l], sem.at[1, l])
        rows_ref[0, l, me] = grad_ref[l, me]
    copies = []
    for l in order:
        blocks_desc(n_emb, grad_ref.at[l], rows_ref.at[0, l], sem.at[0, l], sem.at[1, l]).wait()
        cp = partner_copy(rows_ref.at[0, l], rows_ref.at[1, l], psem.at[0, l], psem.at[1, l])
        cp.start()
        copies.append(cp)
    for cp in copies:
        cp.wait()


def return_rows(n_emb, grads):
    n_layers = grads.shape[0]
    vmem = pl.BlockSpec(memory_space=pltpu.VMEM)
    return pl.pallas_call(
        functools.partial(return_kernel, n_emb),
        out_shape=jax.ShapeDtypeStruct((2,) + grads.shape, F32),
        in_specs=[vmem],
        out_specs=vmem,
        scratch_shapes=[pltpu.SemaphoreType.DMA((2, n_layers)), pltpu.SemaphoreType.DMA((2, n_layers))],
        compiler_params=pltpu.CompilerParams(collective_id=1, has_side_effects=True, vmem_limit_bytes=VMEM_LIMIT),
        name="return_rows",
    )(grads)


def scatter(ids, rows, n_rows):
    _, n_layers, n_emb, _, e = rows.shape

    return pl.pallas_call(
        functools.partial(scatter_kernel, n_layers),
        out_shape=jax.ShapeDtypeStruct((n_layers, n_rows, e), F32),
        in_specs=[pl.BlockSpec(memory_space=pltpu.SMEM), pl.BlockSpec(memory_space=pltpu.VMEM)],
        out_specs=pl.BlockSpec(memory_space=pl.ANY),
        scratch_shapes=[pltpu.VMEM((n_layers, n_rows, e), F32), pltpu.SemaphoreType.DMA((n_layers,))],
        compiler_params=pltpu.CompilerParams(vmem_limit_bytes=VMEM_LIMIT),
        name="scatter",
    )(ids, rows)


def scatter_kernel(n_layers, ids_ref, rows_ref, out_hbm, acc, sem):
    n_rows, e = acc.shape[1:]
    n_emb = rows_ref.shape[2]

    def clear(i, carry):
        for l in range(n_layers):
            acc[l, pl.ds(pl.multiple_of(i * 64, 64), 64), :] = jnp.zeros((64, e), F32)
        return carry

    lax.fori_loop(0, n_rows // 64, clear, 0)

    for half in range(2):
        def block(b, carry):
            base = (half * n_emb + b) * CAP

            def row(k, carry):
                v = ids_ref[base + k] - 1
                for l in range(n_layers):
                    acc[l, pl.ds(v, 1), :] += rows_ref[half, l, b, pl.ds(k, 1), :]
                return carry

            n = jnp.int32(0)
            for k in range(CAP):
                n = n + jnp.minimum(ids_ref[base + k], 1)
            lax.fori_loop(0, n, row, 0)
            return carry

        lax.fori_loop(0, n_emb, block, 0)
    outs = [pltpu.make_async_copy(acc.at[l], out_hbm.at[l], sem.at[l]) for l in range(n_layers)]
    for cp in outs:
        cp.start()
    for cp in outs:
        cp.wait()


def solution(mesh):
    n_emb = mesh.shape["emb"]
    tok_spec = P(("dp", "emb"))
    act_spec = P(("dp", "emb"), None)
    table_spec = P(None, "emb", None)
    full_spec = P(None, None, None)

    def device_body(tok_ids, resid_in, cot_out, tables, w_up, w_down, w_gate, w_proj):
        n_rows = tables.shape[1]
        f = w_up.shape[2]
        tf = 768 if f % 768 == 0 else 256
        fetched, st, recv_ids = fetch(n_emb, tok_ids, tables)
        resid_out, grads = dense(n_emb, resid_in, cot_out, fetched, st, w_up, w_down, w_gate, w_proj, tf)
        rows = return_rows(n_emb, grads)
        ids = recv_ids[:, :, 0, :CAP].reshape(-1)
        return resid_out, scatter(ids, rows, n_rows)

    return jax.shard_map(device_body, mesh=mesh,
                         in_specs=(tok_spec, act_spec, act_spec, table_spec, full_spec, full_spec, full_spec, full_spec),
                         out_specs=(act_spec, table_spec), check_vma=False)
```

```python
import functools
import math

import jax
import jax.numpy as jnp
from jax import lax
from jax.experimental import pallas as pl
from jax.experimental.pallas import tpu as pltpu
from jax.sharding import PartitionSpec as P

NORM_EPS = 1e-6
CAP = 8
BF = jnp.bfloat16
F32 = jnp.float32
MESH_ID = pl.DeviceIdType.MESH
VMEM_LIMIT = 67_043_328
GELU_C = math.sqrt(2.0 / math.pi)


def dot(a, b):
    return jnp.dot(a, b, preferred_element_type=F32)


def dot_nt(a, b):
    return lax.dot_general(a, b, (((1,), (1,)), ((), ())), preferred_element_type=F32)


def dot_tn(a, b):
    return lax.dot_general(a, b, (((0,), (0,)), ((), ())), preferred_element_type=F32)


def iota(shape, axis):
    return lax.broadcasted_iota(jnp.int32, shape, axis)


def gelu_both(x):
    x2 = x * x
    t = jnp.tanh(x * (GELU_C + (GELU_C * 0.044715) * x2))
    hx = 0.5 * x
    s = 0.5 + 0.5 * t
    d = s + hx * (1.0 - t * t) * (GELU_C + (3.0 * GELU_C * 0.044715) * x2)
    return x * s, d


def inv_rms(x):
    return lax.rsqrt(jnp.mean(x * x, axis=-1, keepdims=True) + NORM_EPS)


def peers_barrier(n_emb):
    me, dp = lax.axis_index("emb"), lax.axis_index("dp")
    bar = pltpu.get_barrier_semaphore()

    def tell(k, carry):
        pl.semaphore_signal(bar, inc=1, device_id={"emb": lax.rem(me + k, n_emb)}, device_id_type=MESH_ID)
        return carry

    lax.fori_loop(1, n_emb, tell, 0)
    pl.semaphore_signal(bar, inc=1, device_id={"dp": 1 - dp}, device_id_type=MESH_ID)
    return bar


def send_blocks(n_emb, src, dst, send_sem, recv_sem):
    me = lax.axis_index("emb")

    def one(k, carry):
        to = lax.rem(me + k, n_emb)
        pltpu.make_async_remote_copy(
            src_ref=src.at[to], dst_ref=dst.at[me], send_sem=send_sem, recv_sem=recv_sem,
            device_id={"emb": to}, device_id_type=MESH_ID).start()
        return carry

    lax.fori_loop(1, n_emb, one, 0)


def blocks_desc(n_emb, src, dst, send_sem, recv_sem):
    me = lax.axis_index("emb")
    return pltpu.make_async_remote_copy(
        src_ref=src.at[pl.ds(0, n_emb - 1)], dst_ref=dst.at[pl.ds(0, n_emb - 1)],
        send_sem=send_sem, recv_sem=recv_sem, device_id={"emb": me}, device_id_type=MESH_ID)


def partner_copy(src, dst, send_sem, recv_sem):
    return pltpu.make_async_remote_copy(
        src_ref=src, dst_ref=dst, send_sem=send_sem, recv_sem=recv_sem,
        device_id={"dp": 1 - lax.axis_index("dp")}, device_id_type=MESH_ID)


RING = 6
GROUP = 3


def step_kernel(n_layers, n_emb, ids_ref, resid_hbm, cot_hbm, table_hbm, up_hbm, down_hbm, gate_hbm, proj_hbm,
                out_hbm, rows_hbm, rid_ref,
                wup, wdn, gate, proj, gp, acc, xs, us, cots, hid, gval, gder, fetched,
                table, st, sid, rid, served, fetch_in, grad_out, grad_in,
                upsem, dnsem, ldsem, tsem, isem, psem, fsem, gsem, dsem, wsem):
    me = lax.axis_index("emb")
    n_rows, e = table.shape[1:]
    t, d = acc.shape
    tf = wup.shape[2]
    n_slots = n_emb * CAP
    n_chunks = up_hbm.shape[2] // tf
    n_groups = n_chunks // GROUP
    total = (2 * n_layers - 1) * n_chunks

    def layer_of(g):
        p = g // n_chunks
        return jnp.minimum(p, 2 * n_layers - 1 - p)

    def up_copy(g):
        c, s = lax.rem(g, n_chunks), lax.rem(g, RING)
        return pltpu.make_async_copy(up_hbm.at[layer_of(g), :, pl.ds(pl.multiple_of(c * tf, tf), tf)],
                                     wup.at[s], upsem.at[s])

    def dn_copy(g):
        c, s = lax.rem(g, n_chunks), lax.rem(g, RING)
        return pltpu.make_async_copy(down_hbm.at[layer_of(g), pl.ds(pl.multiple_of(c * tf, tf), tf), :],
                                     wdn.at[s], dnsem.at[s])

    load_x = pltpu.make_async_copy(resid_hbm, xs.at[0], ldsem.at[0])
    load_gate = pltpu.make_async_copy(gate_hbm, gate, ldsem.at[1])
    load_proj = pltpu.make_async_copy(proj_hbm, proj, ldsem.at[2])
    load_cot = pltpu.make_async_copy(cot_hbm, cots, ldsem.at[3])
    load_table = [pltpu.make_async_copy(table_hbm.at[l], table.at[l], tsem.at[l]) for l in range(n_layers)]
    load_x.start()
    load_gate.start()
    for g in range(GROUP):
        up_copy(jnp.int32(g)).start()
        dn_copy(jnp.int32(g)).start()
    for ld in load_table:
        ld.start()
    load_proj.start()
    for g in range(GROUP, RING):
        up_copy(jnp.int32(g)).start()
        dn_copy(jnp.int32(g)).start()
    load_cot.start()
    bar = peers_barrier(n_emb)


    ids = ids_ref[...]
    shift = n_rows.bit_length() - 1
    owner = lax.shift_right_logical(ids, shift)
    local = ids - lax.shift_left(owner, shift) + 1
    own_t = owner == iota((n_emb, t), 0)
    before = (iota((t, t), 0) < iota((t, t), 1)).astype(F32).astype(BF)
    own_f = own_t.astype(F32)
    rank = jnp.sum(own_f * dot(own_f.astype(BF), before), axis=0, keepdims=True).astype(jnp.int32)
    st[...] = (owner * CAP + rank == iota((n_slots, t), 0)).astype(F32).astype(BF)
    rank_t = (rank == iota((128, t), 0)).astype(F32).astype(BF)
    id_hi = jnp.where(own_t, lax.shift_right_logical(local, 6).astype(F32), 0.0).astype(BF)
    id_lo = jnp.where(own_t, jnp.bitwise_and(local, 63).astype(F32), 0.0).astype(BF)
    sid[...] = (64.0 * dot_nt(id_hi, rank_t) + dot_nt(id_lo, rank_t)).astype(jnp.int32).reshape(sid.shape)

    def send_ids():
        pl.semaphore_wait(bar, n_emb)
        send_blocks(n_emb, sid, rid, isem.at[0], isem.at[1])

    ids_to_partner = partner_copy(rid_ref.at[0], rid_ref.at[1], psem.at[0], psem.at[1])

    def serve():
        blocks_desc(n_emb, sid, rid, isem.at[0], isem.at[1]).wait()
        rid[me] = sid[me]
        ids_in = rid[...].reshape(n_emb, 128)
        spread = (lax.shift_right_logical(iota((n_slots, n_emb), 0), 3) == iota((n_slots, n_emb), 1))
        spread = spread.astype(F32).astype(BF)
        hi = lax.shift_right_logical(ids_in, 6).astype(F32).astype(BF)
        lo = jnp.bitwise_and(ids_in, 63).astype(F32).astype(BF)
        pick = jnp.bitwise_and(iota((n_slots, 128), 0), CAP - 1) == iota((n_slots, 128), 1)
        col_hi = jnp.sum(jnp.where(pick, dot(spread, hi), 0.0), axis=1, keepdims=True)
        col_lo = jnp.sum(jnp.where(pick, dot(spread, lo), 0.0), axis=1, keepdims=True)
        col = (64.0 * col_hi + col_lo).astype(jnp.int32) - 1
        chunk = min(1024, n_rows)
        for l in range(n_layers):
            load_table[l].wait()
            sel = None
            for c in range(n_rows // chunk):
                oh = (col == iota((n_slots, chunk), 1) + c * chunk).astype(F32).astype(BF)
                part = dot(oh, table[l, c * chunk:(c + 1) * chunk, :])
                sel = part if sel is None else sel + part
            served[l] = sel.astype(BF).reshape(n_emb, CAP, e)
            send_blocks(n_emb, served.at[l], fetch_in.at[l], fsem.at[0, l], fsem.at[1, l])
        lane = jnp.bitwise_and(iota((n_slots, 128), 0), 127) == iota((n_slots, 128), 1)
        row = (lax.shift_right_logical(iota((8, n_slots), 1), 7) == iota((8, n_slots), 0)).astype(F32).astype(BF)
        flat_hi = dot(row, jnp.where(lane, col_hi, 0.0).astype(BF))
        flat_lo = dot(row, jnp.where(lane, col_lo, 0.0).astype(BF))
        rid_ref[0] = (64.0 * flat_hi + flat_lo).astype(jnp.int32)
        ids_to_partner.start()


    def begin_forward(l):
        x = xs[l].astype(F32)
        us[...] = (x * inv_rms(x)).astype(BF)
        g, der = gelu_both(dot(us[...], gate[l]))
        gval[l] = g
        gder[l] = der
        acc[...] = x

    n_sub = tf // 256

    def fwd_up(l, g, c, k):
        w = wup.at[lax.rem(g, RING)]
        for j in range(n_sub):
            cols = slice(j * 256, (j + 1) * 256)
            h, der = gelu_both(dot(us[...], w[:, cols]))
            hid[k, :, cols] = h.astype(BF)
            gp[lax.rem(l + 1, 2), c, :, cols] = der
        up_copy(g + RING).start()

    def fwd_down(g, k):
        acc[...] += dot(hid[k], wdn[lax.rem(g, RING)])
        dn_copy(g + RING).start()

    def wait_group(g):
        for k in range(GROUP):
            up_copy(g + k).wait()
            dn_copy(g + k).wait()

    def end_forward(l):
        for q in range(n_layers):
            @pl.when(l == q)
            def _():
                blocks_desc(n_emb, served.at[q], fetch_in.at[q], fsem.at[0, q], fsem.at[1, q]).wait()
        fetch_in[l, me] = served[l, me]
        fetched[l] = dot_tn(st[...], fetch_in[l].reshape(n_slots, e)).astype(BF)
        mixed = (gval[l] * fetched[l].astype(F32)).astype(BF)
        xs[l + 1] = (acc[...] + dot(mixed, proj[l])).astype(BF)

    def forward(i, carry):
        l, c0 = i // n_groups, lax.rem(i, n_groups) * GROUP
        g = i * GROUP

        @pl.when(c0 == 0)
        def _():
            begin_forward(l)

        @pl.when(i == 1)
        def _():
            send_ids()

        @pl.when(i == 2)
        def _():
            serve()

        wait_group(g)
        fwd_up(l, g, c0, 0)
        fwd_up(l, g + 1, c0 + 1, 1)
        fwd_down(g, 0)
        fwd_up(l, g + 2, c0 + 2, 2)
        fwd_down(g + 1, 1)
        fwd_down(g + 2, 2)

        @pl.when(c0 == n_chunks - GROUP)
        def _():
            end_forward(l)

        return carry

    load_x.wait()
    load_gate.wait()
    load_proj.wait()
    lax.fori_loop(0, n_layers * n_groups, forward, 0)
    write_out = pltpu.make_async_copy(xs.at[n_layers], out_hbm, wsem.at[0])
    write_out.start()
    load_cot.wait()


    def send_grads(l):
        d_mixed = dot_nt(cots[...], proj[l]).astype(BF).astype(F32)
        rows = gval[l] * d_mixed
        hi = rows.astype(BF)
        rest = rows - hi.astype(F32)
        mid = rest.astype(BF)
        low = (rest - mid.astype(F32)).astype(BF)
        slots = dot(st[...], hi) + dot(st[...], mid) + dot(st[...], low)
        grad_out[l] = slots.reshape(grad_out.shape[1:])
        send_blocks(n_emb, grad_out.at[l], grad_in.at[l], gsem.at[0, l], gsem.at[1, l])
        return d_mixed

    def to_partner(l):
        return partner_copy(grad_in.at[l], rows_hbm.at[1, l], dsem.at[0, l], dsem.at[1, l])

    def to_hbm(l):
        return pltpu.make_async_copy(grad_in.at[l], rows_hbm.at[0, l], wsem.at[1 + l])

    def hand_over(l):
        blocks_desc(n_emb, grad_out.at[l], grad_in.at[l], gsem.at[0, l], gsem.at[1, l]).wait()
        grad_in[l, me] = grad_out[l, me]
        to_partner(l).start()
        to_hbm(l).start()

    def begin_backward(l):
        d_mixed = send_grads(l)
        d_gate = (gder[l] * (d_mixed * fetched[l].astype(F32))).astype(BF)
        us[...] = dot_nt(d_gate, gate[l]).astype(BF)
        acc[...] = jnp.zeros_like(acc)

    def bwd_down(l, g, c, k):
        w = wdn.at[lax.rem(g, RING)]
        for j in range(n_sub):
            cols = slice(j * 256, (j + 1) * 256)
            dh = dot_nt(cots[...], w[cols, :]).astype(BF).astype(F32)
            hid[k, :, cols] = (gp[lax.rem(l + 1, 2), c, :, cols] * dh).astype(BF)

    def bwd_up(g, k):
        acc[...] += dot_nt(hid[k], wup[lax.rem(g, RING)])

    def end_backward(l):
        d_norm = (acc[...].astype(BF).astype(F32) + us[...].astype(F32)).astype(BF).astype(F32)
        x = xs[l].astype(F32)
        r = inv_rms(x)
        dx = r * d_norm - x * (r * r * r * jnp.mean(x * d_norm, axis=-1, keepdims=True))
        cots[...] = (cots[...].astype(F32) + dx).astype(BF)

    def backward(i, carry):
        l, c0 = n_layers - 1 - i // n_groups, lax.rem(i, n_groups) * GROUP
        g = (n_layers * n_groups + i) * GROUP

        @pl.when(c0 == 0)
        def _():
            begin_backward(l)

        wait_group(g)
        bwd_down(l, g, c0, 0)
        bwd_down(l, g + 1, c0 + 1, 1)
        bwd_up(g, 0)

        @pl.when(g + RING < total)
        def _():
            dn_copy(g + RING).start()
            up_copy(g + RING).start()
            dn_copy(g + 1 + RING).start()

        bwd_down(l, g + 2, c0 + 2, 2)
        bwd_up(g + 1, 1)
        bwd_up(g + 2, 2)

        @pl.when(g + RING < total)
        def _():
            up_copy(g + 1 + RING).start()
            dn_copy(g + 2 + RING).start()
            up_copy(g + 2 + RING).start()

        @pl.when(c0 == n_chunks - GROUP)
        def _():
            end_backward(l)
            for q in range(1, n_layers):
                @pl.when(l == q)
                def _():
                    hand_over(q)

        return carry

    lax.fori_loop(0, (n_layers - 1) * n_groups, backward, 0)
    send_grads(0)
    hand_over(0)
    ids_to_partner.wait()
    write_out.wait()
    for l in reversed(range(n_layers)):
        to_hbm(l).wait()
        to_partner(l).wait()


def step(n_emb, tok_ids, resid, cot, tables, w_up, w_down, w_gate, w_proj, tf):
    t, d = resid.shape
    n_layers, n_rows, e = tables.shape
    f = w_up.shape[2]
    n_slots = n_emb * CAP
    vmem, hbm = pl.BlockSpec(memory_space=pltpu.VMEM), pl.BlockSpec(memory_space=pl.ANY)
    dma = pltpu.SemaphoreType.DMA
    return pl.pallas_call(
        functools.partial(step_kernel, n_layers, n_emb),
        out_shape=(jax.ShapeDtypeStruct((t, d), BF),
                   jax.ShapeDtypeStruct((2, n_layers, n_emb, CAP, e), F32),
                   jax.ShapeDtypeStruct((2, 8, 128), jnp.int32)),
        in_specs=[vmem] + [hbm] * 7,
        out_specs=(hbm, hbm, vmem),
        scratch_shapes=[
            pltpu.VMEM((RING, d, tf), BF),
            pltpu.VMEM((RING, tf, d), BF),
            pltpu.VMEM((n_layers, d, e), BF),
            pltpu.VMEM((n_layers, e, d), BF),
            pltpu.VMEM((2, f // tf, t, tf), F32),
            pltpu.VMEM((t, d), F32),
            pltpu.VMEM((n_layers + 1, t, d), BF),
            pltpu.VMEM((t, d), BF),
            pltpu.VMEM((t, d), BF),
            pltpu.VMEM((GROUP, t, tf), BF),
            pltpu.VMEM((n_layers, t, e), F32),
            pltpu.VMEM((n_layers, t, e), F32),
            pltpu.VMEM((n_layers, t, e), BF),
            pltpu.VMEM((n_layers, n_rows, e), BF),
            pltpu.VMEM((n_slots, t), BF),
            pltpu.VMEM((n_emb, 1, 128), jnp.int32),
            pltpu.VMEM((n_emb, 1, 128), jnp.int32),
            pltpu.VMEM((n_layers, n_emb, CAP, e), BF),
            pltpu.VMEM((n_layers, n_emb, CAP, e), BF),
            pltpu.VMEM((n_layers, n_emb, CAP, e), F32),
            pltpu.VMEM((n_layers, n_emb, CAP, e), F32),
            dma((RING,)), dma((RING,)), dma((4,)), dma((n_layers,)), dma((2,)), dma((2,)),
            dma((2, n_layers)), dma((2, n_layers)), dma((2, n_layers)), dma((1 + n_layers,)),
        ],
        compiler_params=pltpu.CompilerParams(collective_id=0, has_side_effects=True, vmem_limit_bytes=VMEM_LIMIT),
        name="step",
    )(tok_ids.reshape(1, t), resid, cot, tables, w_up, w_down, w_gate, w_proj)


def scatter_kernel(n_layers, n_rows, ids_ref, rows_hbm, out_hbm, rows, *scratch):
    acc, (insem, sem) = scratch[:n_layers], scratch[n_layers:]
    e = rows.shape[4]
    n_emb = rows.shape[2]
    load = pltpu.make_async_copy(rows_hbm, rows, insem)
    load.start()

    def clear(i, carry):
        for l in range(n_layers):
            acc[l][pl.ds(pl.multiple_of(i * 64, 64), 64), :] = jnp.zeros((64, e), F32)
        return carry

    lax.fori_loop(0, n_rows // 64, clear, 0)
    load.wait()

    for half in range(2):
        def block(b, carry):
            s = b * CAP
            i, j = lax.shift_right_logical(s, 7), jnp.bitwise_and(s, 127)
            for k in range(0, CAP, 2):
                v, w = ids_ref[half, i, j + k], ids_ref[half, i, j + k + 1]
                v, w = jnp.where(v > 0, v - 1, n_rows), jnp.where(w > 0, w - 1, n_rows + 1)
                same = v == w
                for l in range(n_layers):
                    first, second = rows[half, l, b, k:k + 1, :], rows[half, l, b, k + 1:k + 2, :]
                    at_v, at_w = acc[l][pl.ds(v, 1), :], acc[l][pl.ds(w, 1), :]
                    acc[l][pl.ds(v, 1), :] = at_v + first
                    acc[l][pl.ds(w, 1), :] = at_w + (second + jnp.where(same, first, 0.0))
            return carry

        lax.fori_loop(0, n_emb, block, 0)
    outs = [pltpu.make_async_copy(acc[l].at[pl.ds(0, n_rows)], out_hbm.at[l], sem.at[l]) for l in range(n_layers)]
    for cp in outs:
        cp.start()
    for cp in outs:
        cp.wait()


def scatter(ids, rows, n_rows):
    _, n_layers, n_emb, _, e = rows.shape
    return pl.pallas_call(
        functools.partial(scatter_kernel, n_layers, n_rows),
        out_shape=jax.ShapeDtypeStruct((n_layers, n_rows, e), F32),
        in_specs=[pl.BlockSpec(memory_space=pltpu.SMEM), pl.BlockSpec(memory_space=pl.ANY)],
        out_specs=pl.BlockSpec(memory_space=pl.ANY),
        scratch_shapes=[pltpu.VMEM(rows.shape, F32)] + [pltpu.VMEM((n_rows + 8, e), F32)] * n_layers
        + [pltpu.SemaphoreType.DMA, pltpu.SemaphoreType.DMA((n_layers,))],
        compiler_params=pltpu.CompilerParams(vmem_limit_bytes=VMEM_LIMIT),
        name="scatter",
    )(ids, rows)


def solution(mesh):
    n_emb = mesh.shape["emb"]
    tok_spec = P(("dp", "emb"))
    act_spec = P(("dp", "emb"), None)
    table_spec = P(None, "emb", None)
    full_spec = P(None, None, None)

    def device_body(tok_ids, resid_in, cot_out, tables, w_up, w_down, w_gate, w_proj):
        f = w_up.shape[2]
        tf = 768 if f % (9 * 768) == 0 else 256
        resid_out, rows, ids = step(n_emb, tok_ids, resid_in, cot_out, tables, w_up, w_down, w_gate, w_proj, tf)
        return resid_out, scatter(ids, rows, tables.shape[1])

    return jax.shard_map(device_body, mesh=mesh,
                         in_specs=(tok_spec, act_spec, act_spec, table_spec, full_spec, full_spec, full_spec, full_spec),
                         out_specs=(act_spec, table_spec), check_vma=False)
```

```python
import functools
import math

import jax
import jax.numpy as jnp
from jax import lax
from jax.experimental import pallas as pl
from jax.experimental.pallas import tpu as pltpu
from jax.sharding import PartitionSpec as P

NORM_EPS = 1e-6
CAP = 8
BF = jnp.bfloat16
F32 = jnp.float32
MESH_ID = pl.DeviceIdType.MESH
VMEM_LIMIT = 67_043_328
GELU_C = math.sqrt(2.0 / math.pi)


def dot(a, b):
    return jnp.dot(a, b, preferred_element_type=F32)


def dot_nt(a, b):
    return lax.dot_general(a, b, (((1,), (1,)), ((), ())), preferred_element_type=F32)


def dot_tn(a, b):
    return lax.dot_general(a, b, (((0,), (0,)), ((), ())), preferred_element_type=F32)


def iota(shape, axis):
    return lax.broadcasted_iota(jnp.int32, shape, axis)


def gelu_both(x):
    x2 = x * x
    t = jnp.tanh(x * (GELU_C + (GELU_C * 0.044715) * x2))
    hx = 0.5 * x
    s = 0.5 + 0.5 * t
    d = s + hx * (1.0 - t * t) * (GELU_C + (3.0 * GELU_C * 0.044715) * x2)
    return x * s, d


def inv_rms(x):
    return lax.rsqrt(jnp.mean(x * x, axis=-1, keepdims=True) + NORM_EPS)


def peers_barrier(n_emb):
    me, dp = lax.axis_index("emb"), lax.axis_index("dp")
    bar = pltpu.get_barrier_semaphore()

    def tell(k, carry):
        pl.semaphore_signal(bar, inc=1, device_id={"emb": lax.rem(me + k, n_emb)}, device_id_type=MESH_ID)
        return carry

    lax.fori_loop(1, n_emb, tell, 0)
    pl.semaphore_signal(bar, inc=1, device_id={"dp": 1 - dp}, device_id_type=MESH_ID)
    return bar


def send_blocks(n_emb, src, dst, send_sem, recv_sem):
    me = lax.axis_index("emb")

    def one(k, carry):
        to = lax.rem(me + k, n_emb)
        pltpu.make_async_remote_copy(
            src_ref=src.at[to], dst_ref=dst.at[me], send_sem=send_sem, recv_sem=recv_sem,
            device_id={"emb": to}, device_id_type=MESH_ID).start()
        return carry

    lax.fori_loop(1, n_emb, one, 0)


def blocks_desc(n_emb, src, dst, send_sem, recv_sem):
    me = lax.axis_index("emb")
    return pltpu.make_async_remote_copy(
        src_ref=src.at[pl.ds(0, n_emb - 1)], dst_ref=dst.at[pl.ds(0, n_emb - 1)],
        send_sem=send_sem, recv_sem=recv_sem, device_id={"emb": me}, device_id_type=MESH_ID)


def partner_copy(src, dst, send_sem, recv_sem):
    return pltpu.make_async_remote_copy(
        src_ref=src, dst_ref=dst, send_sem=send_sem, recv_sem=recv_sem,
        device_id={"dp": 1 - lax.axis_index("dp")}, device_id_type=MESH_ID)


RING = 6
GROUP = 3


def step_kernel(n_layers, n_emb, ids_ref, resid_hbm, cot_hbm, table_hbm, up_hbm, down_hbm, gate_hbm, proj_hbm,
                out_hbm, rows_hbm, rid_ref,
                wup, wdn, gate, proj, gp, acc, xs, us, cots, hid, gval, gder, fetched,
                table, st, sid, rid, served, fetch_in, grad_out, grad_in,
                upsem, dnsem, ldsem, tsem, isem, psem, fsem, gsem, dsem, wsem):
    me = lax.axis_index("emb")
    n_rows, e = table.shape[1:]
    t, d = acc.shape
    tf = wup.shape[2]
    n_slots = n_emb * CAP
    n_chunks = up_hbm.shape[2] // tf
    n_groups = n_chunks // GROUP
    total = (2 * n_layers - 1) * n_chunks

    def layer_of(g):
        p = g // n_chunks
        return jnp.minimum(p, 2 * n_layers - 1 - p)

    def chunk_of(g):
        turn = jnp.where(g // n_chunks == n_layers, n_chunks - RING, 0)
        return lax.rem(g + turn, n_chunks)

    def up_copy(g):
        c, s = chunk_of(g), lax.rem(g, RING)
        return pltpu.make_async_copy(up_hbm.at[layer_of(g), :, pl.ds(pl.multiple_of(c * tf, tf), tf)],
                                     wup.at[s], upsem.at[s])

    def dn_copy(g):
        c, s = chunk_of(g), lax.rem(g, RING)
        return pltpu.make_async_copy(down_hbm.at[layer_of(g), pl.ds(pl.multiple_of(c * tf, tf), tf), :],
                                     wdn.at[s], dnsem.at[s])

    load_x = pltpu.make_async_copy(resid_hbm, xs.at[0], ldsem.at[0])
    load_cot = pltpu.make_async_copy(cot_hbm, cots, ldsem.at[1])
    load_proj = pltpu.make_async_copy(proj_hbm, proj, ldsem.at[2])
    load_gate = [pltpu.make_async_copy(gate_hbm.at[l], gate.at[l], ldsem.at[3 + l]) for l in range(n_layers)]
    load_table = [pltpu.make_async_copy(table_hbm.at[l], table.at[l], tsem.at[l]) for l in range(n_layers)]
    load_x.start()
    load_gate[0].start()
    for g in range(RING):
        up_copy(jnp.int32(g)).start()
        dn_copy(jnp.int32(g)).start()
    for ld in load_table + [load_proj] + load_gate[1:] + [load_cot]:
        ld.start()
    bar = peers_barrier(n_emb)


    ids = ids_ref[...]
    shift = n_rows.bit_length() - 1
    owner = lax.shift_right_logical(ids, shift)
    local = ids - lax.shift_left(owner, shift) + 1
    own_t = owner == iota((n_emb, t), 0)
    before = (iota((t, t), 0) < iota((t, t), 1)).astype(F32).astype(BF)
    own_f = own_t.astype(F32)
    rank = jnp.sum(own_f * dot(own_f.astype(BF), before), axis=0, keepdims=True).astype(jnp.int32)
    st[...] = (owner * CAP + rank == iota((n_slots, t), 0)).astype(F32).astype(BF)
    rank_t = (rank == iota((128, t), 0)).astype(F32).astype(BF)
    id_hi = jnp.where(own_t, lax.shift_right_logical(local, 6).astype(F32), 0.0).astype(BF)
    id_lo = jnp.where(own_t, jnp.bitwise_and(local, 63).astype(F32), 0.0).astype(BF)
    sid[...] = (64.0 * dot_nt(id_hi, rank_t) + dot_nt(id_lo, rank_t)).astype(jnp.int32).reshape(sid.shape)

    def send_ids():
        pl.semaphore_wait(bar, n_emb)
        send_blocks(n_emb, sid, rid, isem.at[0], isem.at[1])

    ids_to_partner = partner_copy(rid_ref.at[0], rid_ref.at[1], psem.at[0], psem.at[1])

    def serve():
        blocks_desc(n_emb, sid, rid, isem.at[0], isem.at[1]).wait()
        rid[me] = sid[me]
        ids_in = rid[...].reshape(n_emb, 128)
        spread = (lax.shift_right_logical(iota((n_slots, n_emb), 0), 3) == iota((n_slots, n_emb), 1))
        spread = spread.astype(F32).astype(BF)
        hi = lax.shift_right_logical(ids_in, 6).astype(F32).astype(BF)
        lo = jnp.bitwise_and(ids_in, 63).astype(F32).astype(BF)
        pick = jnp.bitwise_and(iota((n_slots, 128), 0), CAP - 1) == iota((n_slots, 128), 1)
        col_hi = jnp.sum(jnp.where(pick, dot(spread, hi), 0.0), axis=1, keepdims=True)
        col_lo = jnp.sum(jnp.where(pick, dot(spread, lo), 0.0), axis=1, keepdims=True)
        col = (64.0 * col_hi + col_lo).astype(jnp.int32) - 1
        chunk = min(1024, n_rows)
        for l in range(n_layers):
            load_table[l].wait()
            sel = None
            for c in range(n_rows // chunk):
                oh = (col == iota((n_slots, chunk), 1) + c * chunk).astype(F32).astype(BF)
                part = dot(oh, table[l, c * chunk:(c + 1) * chunk, :])
                sel = part if sel is None else sel + part
            served[l] = sel.astype(BF).reshape(n_emb, CAP, e)
            send_blocks(n_emb, served.at[l], fetch_in.at[l], fsem.at[0, l], fsem.at[1, l])
        lane = jnp.bitwise_and(iota((n_slots, 128), 0), 127) == iota((n_slots, 128), 1)
        row = (lax.shift_right_logical(iota((8, n_slots), 1), 7) == iota((8, n_slots), 0)).astype(F32).astype(BF)
        flat_hi = dot(row, jnp.where(lane, col_hi, 0.0).astype(BF))
        flat_lo = dot(row, jnp.where(lane, col_lo, 0.0).astype(BF))
        flat = (64.0 * flat_hi + flat_lo).astype(jnp.int32) - 1
        spare = n_rows + jnp.bitwise_and(iota(flat.shape, 1), 1)
        rid_ref[0] = jnp.where(flat < 0, spare, flat)
        ids_to_partner.start()


    def begin_forward(l):
        x = xs[l].astype(F32)
        us[...] = (x * inv_rms(x)).astype(BF)
        g, der = gelu_both(dot(us[...], gate[l]))
        gval[l] = g
        gder[l] = der
        acc[...] = x

    n_sub = tf // 256

    def fwd_up(l, g, c, k, more):
        w = wup.at[lax.rem(g, RING)]
        for j in range(n_sub):
            cols = slice(j * 256, (j + 1) * 256)
            h, der = gelu_both(dot(us[...], w[:, cols]))
            hid[k, :, cols] = h.astype(BF)
            gp[lax.rem(l + 1, 2), c, :, cols] = der
        if more:
            up_copy(g + RING).start()

    def fwd_down(g, k, more):
        acc[...] += dot(hid[k], wdn[lax.rem(g, RING)])
        if more:
            dn_copy(g + RING).start()

    def wait_group(g):
        for k in range(GROUP):
            up_copy(g + k).wait()
            dn_copy(g + k).wait()

    def end_forward(l):
        for q in range(n_layers):
            @pl.when(l == q)
            def _():
                blocks_desc(n_emb, served.at[q], fetch_in.at[q], fsem.at[0, q], fsem.at[1, q]).wait()
        @pl.when(l == 0)
        def _():
            for ld in [load_proj] + load_gate[1:]:
                ld.wait()

        fetch_in[l, me] = served[l, me]
        fetched[l] = dot_tn(st[...], fetch_in[l].reshape(n_slots, e)).astype(BF)
        mixed = (gval[l] * fetched[l].astype(F32)).astype(BF)
        xs[l + 1] = (acc[...] + dot(mixed, proj[l])).astype(BF)

    def forward(more, i, carry):
        l, c0 = i // n_groups, lax.rem(i, n_groups) * GROUP
        g = i * GROUP

        if more:
            @pl.when(c0 == 0)
            def _():
                begin_forward(l)

            @pl.when(i == 2)
            def _():
                serve()

        wait_group(g)
        fwd_up(l, g, c0, 0, more)
        fwd_up(l, g + 1, c0 + 1, 1, more)
        fwd_down(g, 0, more)
        fwd_up(l, g + 2, c0 + 2, 2, more)
        fwd_down(g + 1, 1, more)
        fwd_down(g + 2, 2, more)

        @pl.when(c0 == n_chunks - GROUP)
        def _():
            end_forward(l)

        return carry

    load_x.wait()
    load_gate[0].wait()
    begin_forward(0)
    for k in range(GROUP):
        g = jnp.int32(k)
        up_copy(g).wait()
        fwd_up(0, g, k, k, True)
        dn_copy(g).wait()
        fwd_down(g, k, True)
    send_ids()
    kept = n_layers * n_groups - RING // GROUP
    lax.fori_loop(1, kept, functools.partial(forward, True), 0)
    lax.fori_loop(kept, n_layers * n_groups, functools.partial(forward, False), 0)
    write_out = pltpu.make_async_copy(xs.at[n_layers], out_hbm, wsem.at[0])
    write_out.start()
    load_cot.wait()


    def send_grads(l):
        d_mixed = dot_nt(cots[...], proj[l]).astype(BF).astype(F32)
        rows = gval[l] * d_mixed
        hi = rows.astype(BF)
        rest = rows - hi.astype(F32)
        mid = rest.astype(BF)
        low = (rest - mid.astype(F32)).astype(BF)
        slots = dot(st[...], hi) + dot(st[...], mid) + dot(st[...], low)
        grad_out[l] = slots.reshape(grad_out.shape[1:])
        send_blocks(n_emb, grad_out.at[l], grad_in.at[l], gsem.at[0, l], gsem.at[1, l])
        return d_mixed

    def to_partner(l):
        return partner_copy(grad_in.at[l], rows_hbm.at[1, l], dsem.at[0, l], dsem.at[1, l])

    def to_hbm(l):
        return pltpu.make_async_copy(grad_in.at[l], rows_hbm.at[0, l], wsem.at[1 + l])

    def hand_over(l):
        blocks_desc(n_emb, grad_out.at[l], grad_in.at[l], gsem.at[0, l], gsem.at[1, l]).wait()
        grad_in[l, me] = grad_out[l, me]
        to_partner(l).start()
        to_hbm(l).start()

    def begin_backward(l):
        d_mixed = send_grads(l)
        d_gate = (gder[l] * (d_mixed * fetched[l].astype(F32))).astype(BF)
        us[...] = dot_nt(d_gate, gate[l]).astype(BF)
        acc[...] = jnp.zeros_like(acc)

    def bwd_down(l, g, c, k):
        w = wdn.at[lax.rem(g, RING)]
        for j in range(n_sub):
            cols = slice(j * 256, (j + 1) * 256)
            dh = dot_nt(cots[...], w[cols, :]).astype(BF).astype(F32)
            hid[k, :, cols] = (gp[lax.rem(l + 1, 2), c, :, cols] * dh).astype(BF)

    def bwd_up(g, k):
        acc[...] += dot_nt(hid[k], wup[lax.rem(g, RING)])

    def end_backward(l):
        d_norm = (acc[...].astype(BF).astype(F32) + us[...].astype(F32)).astype(BF).astype(F32)
        x = xs[l].astype(F32)
        r = inv_rms(x)
        dx = r * d_norm - x * (r * r * r * jnp.mean(x * d_norm, axis=-1, keepdims=True))
        cots[...] = (cots[...].astype(F32) + dx).astype(BF)

    def backward(i, carry):
        l, place = n_layers - 1 - i // n_groups, lax.rem(i, n_groups)
        g = (n_layers * n_groups + i) * GROUP
        c0 = chunk_of(g)

        @pl.when(place == 0)
        def _():
            begin_backward(l)

        @pl.when(i >= RING // GROUP)
        def _():
            wait_group(g)

        bwd_down(l, g, c0, 0)
        bwd_down(l, g + 1, c0 + 1, 1)
        bwd_up(g, 0)

        @pl.when(g + RING < total)
        def _():
            dn_copy(g + RING).start()
            up_copy(g + RING).start()
            dn_copy(g + 1 + RING).start()

        bwd_down(l, g + 2, c0 + 2, 2)
        bwd_up(g + 1, 1)
        bwd_up(g + 2, 2)

        @pl.when(g + RING < total)
        def _():
            up_copy(g + 1 + RING).start()
            dn_copy(g + 2 + RING).start()
            up_copy(g + 2 + RING).start()

        @pl.when(place == n_groups - 1)
        def _():
            end_backward(l)
            for q in range(1, n_layers):
                @pl.when(l == q)
                def _():
                    hand_over(q)

        return carry

    lax.fori_loop(0, (n_layers - 1) * n_groups, backward, 0)
    send_grads(0)
    hand_over(0)
    ids_to_partner.wait()
    write_out.wait()
    for l in reversed(range(n_layers)):
        to_hbm(l).wait()
        to_partner(l).wait()


def step(n_emb, tok_ids, resid, cot, tables, w_up, w_down, w_gate, w_proj, tf):
    t, d = resid.shape
    n_layers, n_rows, e = tables.shape
    f = w_up.shape[2]
    n_slots = n_emb * CAP
    vmem, hbm = pl.BlockSpec(memory_space=pltpu.VMEM), pl.BlockSpec(memory_space=pl.ANY)
    dma = pltpu.SemaphoreType.DMA
    return pl.pallas_call(
        functools.partial(step_kernel, n_layers, n_emb),
        out_shape=(jax.ShapeDtypeStruct((t, d), BF),
                   jax.ShapeDtypeStruct((2, n_layers, n_emb, CAP, e), F32),
                   jax.ShapeDtypeStruct((2, 8, 128), jnp.int32)),
        in_specs=[vmem] + [hbm] * 7,
        out_specs=(hbm, hbm, vmem),
        scratch_shapes=[
            pltpu.VMEM((RING, d, tf), BF),
            pltpu.VMEM((RING, tf, d), BF),
            pltpu.VMEM((n_layers, d, e), BF),
            pltpu.VMEM((n_layers, e, d), BF),
            pltpu.VMEM((2, f // tf, t, tf), F32),
            pltpu.VMEM((t, d), F32),
            pltpu.VMEM((n_layers + 1, t, d), BF),
            pltpu.VMEM((t, d), BF),
            pltpu.VMEM((t, d), BF),
            pltpu.VMEM((GROUP, t, tf), BF),
            pltpu.VMEM((n_layers, t, e), F32),
            pltpu.VMEM((n_layers, t, e), F32),
            pltpu.VMEM((n_layers, t, e), BF),
            pltpu.VMEM((n_layers, n_rows, e), BF),
            pltpu.VMEM((n_slots, t), BF),
            pltpu.VMEM((n_emb, 1, 128), jnp.int32),
            pltpu.VMEM((n_emb, 1, 128), jnp.int32),
            pltpu.VMEM((n_layers, n_emb, CAP, e), BF),
            pltpu.VMEM((n_layers, n_emb, CAP, e), BF),
            pltpu.VMEM((n_layers, n_emb, CAP, e), F32),
            pltpu.VMEM((n_layers, n_emb, CAP, e), F32),
            dma((RING,)), dma((RING,)), dma((3 + n_layers,)), dma((n_layers,)), dma((2,)), dma((2,)),
            dma((2, n_layers)), dma((2, n_layers)), dma((2, n_layers)), dma((1 + n_layers,)),
        ],
        compiler_params=pltpu.CompilerParams(collective_id=0, has_side_effects=True, vmem_limit_bytes=VMEM_LIMIT),
        name="step",
    )(tok_ids.reshape(1, t), resid, cot, tables, w_up, w_down, w_gate, w_proj)


def scatter_kernel(n_layers, n_rows, ids_ref, rows_hbm, x_hbm, out_hbm, x_out, rows, x, *scratch):
    acc, (insem, xsem, sem) = scratch[:n_layers], scratch[n_layers:]
    e = rows.shape[4]
    n_emb = rows.shape[2]
    loads = [pltpu.make_async_copy(rows_hbm.at[h], rows.at[h], insem.at[h]) for h in range(2)]
    x_in = pltpu.make_async_copy(x_hbm, x, xsem.at[0])
    x_back = pltpu.make_async_copy(x, x_out, xsem.at[1])
    for ld in loads + [x_in]:
        ld.start()

    def clear(i, carry):
        for l in range(n_layers):
            acc[l][pl.ds(pl.multiple_of(i * 64, 64), 64), :] = jnp.zeros((64, e), F32)
        return carry

    lax.fori_loop(0, n_rows // 64, clear, 0)
    per_row = min(128 // CAP, n_emb)

    for half in range(2):
        loads[half].wait()
        if half == 1:
            x_in.wait()
            x_back.start()
        for i in range(n_emb // per_row):
            def block(p, carry):
                b = i * per_row + p
                for k in range(0, CAP, 2):
                    v, w = ids_ref[half, i, p * CAP + k], ids_ref[half, i, p * CAP + k + 1]
                    same = v == w
                    for l in range(n_layers):
                        first, second = rows[half, l, b, k:k + 1, :], rows[half, l, b, k + 1:k + 2, :]
                        at_v, at_w = acc[l][pl.ds(v, 1), :], acc[l][pl.ds(w, 1), :]
                        acc[l][pl.ds(v, 1), :] = at_v + first
                        acc[l][pl.ds(w, 1), :] = at_w + (second + jnp.where(same, first, 0.0))
                return carry

            lax.fori_loop(0, per_row, block, 0)
    outs = [pltpu.make_async_copy(acc[l].at[pl.ds(0, n_rows)], out_hbm.at[l], sem.at[l]) for l in range(n_layers)]
    for cp in outs:
        cp.start()
    for cp in outs + [x_back]:
        cp.wait()


def scatter(ids, rows, x, n_rows):
    _, n_layers, n_emb, _, e = rows.shape
    hbm = pl.BlockSpec(memory_space=pl.ANY)
    return pl.pallas_call(
        functools.partial(scatter_kernel, n_layers, n_rows),
        out_shape=(jax.ShapeDtypeStruct((n_layers, n_rows, e), F32), jax.ShapeDtypeStruct(x.shape, x.dtype)),
        in_specs=[pl.BlockSpec(memory_space=pltpu.SMEM), hbm, hbm],
        out_specs=(hbm, hbm),
        scratch_shapes=[pltpu.VMEM(rows.shape, F32), pltpu.VMEM(x.shape, x.dtype)]
        + [pltpu.VMEM((n_rows + 8, e), F32)] * n_layers
        + [pltpu.SemaphoreType.DMA((2,)), pltpu.SemaphoreType.DMA((2,)), pltpu.SemaphoreType.DMA((n_layers,))],
        compiler_params=pltpu.CompilerParams(vmem_limit_bytes=VMEM_LIMIT),
        name="scatter",
    )(ids, rows, x)


def solution(mesh):
    n_emb = mesh.shape["emb"]
    tok_spec = P(("dp", "emb"))
    act_spec = P(("dp", "emb"), None)
    table_spec = P(None, "emb", None)
    full_spec = P(None, None, None)

    def device_body(tok_ids, resid_in, cot_out, tables, w_up, w_down, w_gate, w_proj):
        f = w_up.shape[2]
        tf = 768 if f % (9 * 768) == 0 else 256
        resid_out, rows, ids = step(n_emb, tok_ids, resid_in, cot_out, tables, w_up, w_down, w_gate, w_proj, tf)
        d_tables, resid_out = scatter(ids, rows, resid_out, tables.shape[1])
        return resid_out, d_tables

    return jax.shard_map(device_body, mesh=mesh,
                         in_specs=(tok_spec, act_spec, act_spec, table_spec, full_spec, full_spec, full_spec, full_spec),
                         out_specs=(act_spec, table_spec), check_vma=False)
```

```python
import functools
import math

import jax
import jax.numpy as jnp
from jax import lax
from jax.experimental import pallas as pl
from jax.experimental.pallas import tpu as pltpu
from jax.sharding import PartitionSpec as P

NORM_EPS = 1e-6
CAP = 8
BF = jnp.bfloat16
F32 = jnp.float32
MESH_ID = pl.DeviceIdType.MESH
VMEM_LIMIT = 67_043_328
GELU_C = math.sqrt(2.0 / math.pi)


def dot(a, b):
    return jnp.dot(a, b, preferred_element_type=F32)


def dot_nt(a, b):
    return lax.dot_general(a, b, (((1,), (1,)), ((), ())), preferred_element_type=F32)


def dot_tn(a, b):
    return lax.dot_general(a, b, (((0,), (0,)), ((), ())), preferred_element_type=F32)


def iota(shape, axis):
    return lax.broadcasted_iota(jnp.int32, shape, axis)


def gelu_both(x):
    x2 = x * x
    t = jnp.tanh(x * (GELU_C + (GELU_C * 0.044715) * x2))
    hx = 0.5 * x
    s = 0.5 + 0.5 * t
    d = s + hx * (1.0 - t * t) * (GELU_C + (3.0 * GELU_C * 0.044715) * x2)
    return x * s, d


def inv_rms(x):
    return lax.rsqrt(jnp.mean(x * x, axis=-1, keepdims=True) + NORM_EPS)


def peers_barrier(n_emb):
    me, dp = lax.axis_index("emb"), lax.axis_index("dp")
    bar = pltpu.get_barrier_semaphore()

    def tell(k, carry):
        pl.semaphore_signal(bar, inc=1, device_id={"emb": lax.rem(me + k, n_emb)}, device_id_type=MESH_ID)
        return carry

    lax.fori_loop(1, n_emb, tell, 0)
    pl.semaphore_signal(bar, inc=1, device_id={"dp": 1 - dp}, device_id_type=MESH_ID)
    return bar


def send_blocks(n_emb, src, dst, send_sem, recv_sem):
    me = lax.axis_index("emb")

    def one(k, carry):
        to = lax.rem(me + k, n_emb)
        pltpu.make_async_remote_copy(
            src_ref=src.at[to], dst_ref=dst.at[me], send_sem=send_sem, recv_sem=recv_sem,
            device_id={"emb": to}, device_id_type=MESH_ID).start()
        return carry

    lax.fori_loop(1, n_emb, one, 0)


def blocks_desc(n_emb, src, dst, send_sem, recv_sem):
    me = lax.axis_index("emb")
    return pltpu.make_async_remote_copy(
        src_ref=src.at[pl.ds(0, n_emb - 1)], dst_ref=dst.at[pl.ds(0, n_emb - 1)],
        send_sem=send_sem, recv_sem=recv_sem, device_id={"emb": me}, device_id_type=MESH_ID)


def partner_copy(src, dst, send_sem, recv_sem):
    return pltpu.make_async_remote_copy(
        src_ref=src, dst_ref=dst, send_sem=send_sem, recv_sem=recv_sem,
        device_id={"dp": 1 - lax.axis_index("dp")}, device_id_type=MESH_ID)


RING = 6
GROUP = 3


def step_kernel(n_layers, n_emb, ids_ref, resid_hbm, cot_hbm, table_hbm, up_hbm, down_hbm, gate_hbm, proj_hbm,
                out_hbm, rows_hbm, rid_ref,
                wup, wdn, gate, proj, gp, acc, xs, us, cots, hid, gval, gder, fetched,
                table, st, sid, rid, served, fetch_in, grad_out, grad_in,
                ringsem, ldsem, tsem, isem, psem, fsem, gsem, dsem, wsem, msem):
    me = lax.axis_index("emb")
    n_rows, e = table.shape[1:]
    t_chunk = min(1024, n_rows)
    t, d = acc.shape
    tf = wup.shape[2]
    n_slots = n_emb * CAP
    n_chunks = up_hbm.shape[2] // tf
    n_groups = n_chunks // GROUP
    total = (2 * n_layers - 1) * n_chunks

    def layer_of(g):
        if isinstance(g, int):
            return 0
        p = g // n_chunks
        return jnp.minimum(p, 2 * n_layers - 1 - p)

    def chunk_of(g):
        if isinstance(g, int):
            return g
        turn = jnp.where(g // n_chunks == n_layers, n_chunks - RING, 0)
        return lax.rem(g + turn, n_chunks)

    def slot_of(g):
        return g % RING if isinstance(g, int) else lax.rem(g, RING)

    def ring_sem(g):
        if isinstance(g, int) and g < GROUP:
            return ringsem.at[2 + min(g, 1)]
        return ringsem.at[lax.rem(g // GROUP, 2)]

    def up_copy(g):
        c, s = chunk_of(g), slot_of(g)
        return pltpu.make_async_copy(up_hbm.at[layer_of(g), :, pl.ds(c * tf if isinstance(c, int) else pl.multiple_of(c * tf, tf), tf)],
                                     wup.at[s], ring_sem(g))

    def dn_copy(g):
        c, s = chunk_of(g), slot_of(g)
        return pltpu.make_async_copy(down_hbm.at[layer_of(g), pl.ds(c * tf if isinstance(c, int) else pl.multiple_of(c * tf, tf), tf), :],
                                     wdn.at[s], ring_sem(g))

    load_x = pltpu.make_async_copy(resid_hbm, xs.at[0], ldsem.at[0])
    load_cot = pltpu.make_async_copy(cot_hbm, cots, ldsem.at[1])
    load_proj = pltpu.make_async_copy(proj_hbm, proj, ldsem.at[2])
    load_gate = [pltpu.make_async_copy(gate_hbm.at[l], gate.at[l], ldsem.at[3 + l]) for l in range(n_layers)]
    load_table = [pltpu.make_async_copy(table_hbm.at[l], table.at[l % 2], tsem.at[l]) for l in range(min(n_layers, 2))]
    load_x.start()
    load_gate[0].start()
    for g in range(RING):
        up_copy(g).start()
        dn_copy(g).start()
    for ld in load_table + [load_proj] + load_gate[1:] + [load_cot]:
        ld.start()
    bar = peers_barrier(n_emb)


    ids = ids_ref[...]
    shift = n_rows.bit_length() - 1
    owner = lax.shift_right_logical(ids, shift)
    local = ids - lax.shift_left(owner, shift) + 1
    own_t = owner == iota((n_emb, t), 0)
    before = (iota((t, t), 0) < iota((t, t), 1)).astype(F32).astype(BF)
    own_f = own_t.astype(F32)
    rank = jnp.sum(own_f * dot(own_f.astype(BF), before), axis=0, keepdims=True).astype(jnp.int32)
    st[...] = (owner * CAP + rank == iota((n_slots, t), 0)).astype(F32).astype(BF)
    rank_t = (rank == iota((128, t), 0)).astype(F32).astype(BF)
    id_hi = jnp.where(own_t, lax.shift_right_logical(local, 6).astype(F32), 0.0).astype(BF)
    id_lo = jnp.where(own_t, jnp.bitwise_and(local, 63).astype(F32), 0.0).astype(BF)
    sid[...] = (64.0 * dot_nt(id_hi, rank_t) + dot_nt(id_lo, rank_t)).astype(jnp.int32).reshape(sid.shape)

    def send_ids():
        pl.semaphore_wait(bar, n_emb)
        send_blocks(n_emb, sid, rid, isem.at[0], isem.at[1])

    ids_to_partner = partner_copy(rid_ref.at[0], rid_ref.at[1], psem.at[0], psem.at[1])

    def serve():
        blocks_desc(n_emb, sid, rid, isem.at[0], isem.at[1]).wait()
        rid[me] = sid[me]
        ids_in = rid[...].reshape(n_emb, 128)
        spread = (lax.shift_right_logical(iota((n_slots, n_emb), 0), 3) == iota((n_slots, n_emb), 1))
        spread = spread.astype(F32).astype(BF)
        hi = lax.shift_right_logical(ids_in, 6).astype(F32).astype(BF)
        lo = jnp.bitwise_and(ids_in, 63).astype(F32).astype(BF)
        pick = jnp.bitwise_and(iota((n_slots, 128), 0), CAP - 1) == iota((n_slots, 128), 1)
        col_hi = jnp.sum(jnp.where(pick, dot(spread, hi), 0.0), axis=1, keepdims=True)
        col_lo = jnp.sum(jnp.where(pick, dot(spread, lo), 0.0), axis=1, keepdims=True)
        col = (64.0 * col_hi + col_lo).astype(jnp.int32) - 1
        chunk = t_chunk
        for l in range(n_layers):
            pltpu.make_async_copy(table_hbm.at[l], table.at[l % 2], tsem.at[l]).wait()
            sel = None
            for c in range(n_rows // chunk):
                oh = (col == iota((n_slots, chunk), 1) + c * chunk).astype(F32).astype(BF)
                part = dot(oh, table[l % 2, c * chunk:(c + 1) * chunk, :])
                if l + 2 < n_layers:
                    piece = pl.ds(c * chunk, chunk)
                    pltpu.make_async_copy(table_hbm.at[l + 2, piece], table.at[l % 2, piece], tsem.at[l + 2]).start()
                sel = part if sel is None else sel + part
            served[l] = sel.astype(BF).reshape(n_emb, CAP, e)
            send_blocks(n_emb, served.at[l], fetch_in.at[l], fsem.at[0, l], fsem.at[1, l])
        lane = jnp.bitwise_and(iota((n_slots, 128), 0), 127) == iota((n_slots, 128), 1)
        row = (lax.shift_right_logical(iota((8, n_slots), 1), 7) == iota((8, n_slots), 0)).astype(F32).astype(BF)
        flat_hi = dot(row, jnp.where(lane, col_hi, 0.0).astype(BF))
        flat_lo = dot(row, jnp.where(lane, col_lo, 0.0).astype(BF))
        flat = (64.0 * flat_hi + flat_lo).astype(jnp.int32) - 1
        spare = n_rows + jnp.bitwise_and(iota(flat.shape, 1), 1)
        rid_ref[0] = jnp.where(flat < 0, spare, flat)
        ids_to_partner.start()

    def send_rows(l, rows):
        hi = rows.astype(BF)
        rest = rows - hi.astype(F32)
        mid = rest.astype(BF)
        low = (rest - mid.astype(F32)).astype(BF)
        slots = dot(st[...], hi) + dot(st[...], mid) + dot(st[...], low)
        grad_out[l] = slots.reshape(grad_out.shape[1:])
        send_blocks(n_emb, grad_out.at[l], grad_in.at[l], gsem.at[0, l], gsem.at[1, l])


    def begin_forward(l):
        x = xs[l].astype(F32)
        us[...] = (x * inv_rms(x)).astype(BF)
        g, der = gelu_both(dot(us[...], gate[l]))
        gval[l] = g
        gder[l] = der
        acc[...] = x

    n_sub = tf // 256

    def fwd_up(l, g, c, k, more):
        w = wup.at[lax.rem(g, RING)]
        for j in range(n_sub):
            cols = slice(j * 256, (j + 1) * 256)
            h, der = gelu_both(dot(us[...], w[:, cols]))
            hid[k, :, cols] = h.astype(BF)
            gp[lax.rem(l + 1, 2), c, :, cols] = der
        if more:
            up_copy(g + RING).start()

    def fwd_down(g, k, more):
        acc[...] += dot(hid[k], wdn[lax.rem(g, RING)])
        if more:
            dn_copy(g + RING).start()

    def wait_chunks(n, sem):
        pltpu.make_async_copy(wup.at[pl.ds(0, 2 * n)], wup.at[pl.ds(0, 2 * n)], sem).wait()

    def wait_group(g):
        wait_chunks(GROUP, ring_sem(g))

    def end_forward(l):
        for q in range(n_layers):
            @pl.when(l == q)
            def _():
                blocks_desc(n_emb, served.at[q], fetch_in.at[q], fsem.at[0, q], fsem.at[1, q]).wait()
        @pl.when(l == 0)
        def _():
            for ld in [load_proj] + load_gate[1:]:
                ld.wait()

        fetch_in[l, me] = served[l, me]
        fetched[l] = dot_tn(st[...], fetch_in[l].reshape(n_slots, e)).astype(BF)
        mixed = (gval[l] * fetched[l].astype(F32)).astype(BF)
        xs[lax.rem(l + 1, n_layers)] = (acc[...] + dot(mixed, proj[l])).astype(BF)

    def forward(more, i, carry):
        l, c0 = i // n_groups, lax.rem(i, n_groups) * GROUP
        g = i * GROUP

        if more:
            @pl.when(c0 == 0)
            def _():
                begin_forward(l)

            @pl.when(i == 2)
            def _():
                serve()

            @pl.when(i == n_groups + 2)
            def _():
                send_rows(0, gval[0])

        wait_group(g)
        fwd_up(l, g, c0, 0, more)
        fwd_up(l, g + 1, c0 + 1, 1, more)
        fwd_down(g, 0, more)
        fwd_up(l, g + 2, c0 + 2, 2, more)
        fwd_down(g + 1, 1, more)
        fwd_down(g + 2, 2, more)

        @pl.when(c0 == n_chunks - GROUP)
        def _():
            end_forward(l)

        return carry

    load_x.wait()
    load_gate[0].wait()
    begin_forward(0)
    wait_chunks(1, ringsem.at[2])
    fwd_up(0, jnp.int32(0), 0, 0, True)
    fwd_down(jnp.int32(0), 0, True)
    wait_chunks(GROUP - 1, ringsem.at[3])
    for k in range(1, GROUP):
        fwd_up(0, jnp.int32(k), k, k, True)
    for k in range(1, GROUP):
        fwd_down(jnp.int32(k), k, True)
    send_ids()
    kept = n_layers * n_groups - RING // GROUP
    lax.fori_loop(1, kept, functools.partial(forward, True), 0)
    lax.fori_loop(kept, n_layers * n_groups, functools.partial(forward, False), 0)
    write_out = pltpu.make_async_copy(xs.at[0], out_hbm, wsem.at[0])
    write_out.start()
    load_cot.wait()


    def mixed_grad(l):
        return dot_nt(cots[...], proj[l]).astype(BF)

    def send_grads(l):
        d_mixed = mixed_grad(l).astype(F32)
        send_rows(l, gval[l] * d_mixed)
        return d_mixed

    mixed_out, mixed_in = served.at[0], fetch_in.at[0]

    def to_partner(l):
        return partner_copy(grad_in.at[l], rows_hbm.at[1, l], dsem.at[0, l], dsem.at[1, l])

    def to_hbm(l):
        return pltpu.make_async_copy(grad_in.at[l], rows_hbm.at[0, l], wsem.at[1 + l])

    def mixed_desc():
        return blocks_desc(n_emb, mixed_out, mixed_in, msem.at[0], msem.at[1])

    def hand_over(l):
        blocks_desc(n_emb, grad_out.at[l], grad_in.at[l], gsem.at[0, l], gsem.at[1, l]).wait()
        grad_in[l, me] = grad_out[l, me]
        if l == 0:
            mixed_desc().wait()
            mixed_in[me] = mixed_out[me]
            grad_in[0] = grad_in[0] * mixed_in[...].astype(F32)
        to_partner(l).start()
        to_hbm(l).start()

    def begin_backward(l):
        d_mixed = send_grads(l)
        for q in range(2, n_layers):
            @pl.when(l == q - 1)
            def _():
                hand_over(q)

        d_gate = (gder[l] * (d_mixed * fetched[l].astype(F32))).astype(BF)
        us[...] = dot_nt(d_gate, gate[l]).astype(BF)
        acc[...] = jnp.zeros_like(acc)

    def bwd_down(l, g, c, k):
        w = wdn.at[lax.rem(g, RING)]
        for j in range(n_sub):
            cols = slice(j * 256, (j + 1) * 256)
            dh = dot_nt(cots[...], w[cols, :]).astype(BF).astype(F32)
            hid[k, :, cols] = (gp[lax.rem(l + 1, 2), c, :, cols] * dh).astype(BF)

    def bwd_up(g, k):
        acc[...] += dot_nt(hid[k], wup[lax.rem(g, RING)])

    def end_backward(l):
        d_norm = (acc[...].astype(BF).astype(F32) + us[...].astype(F32)).astype(BF).astype(F32)
        x = xs[l].astype(F32)
        r = inv_rms(x)
        dx = r * d_norm - x * (r * r * r * jnp.mean(x * d_norm, axis=-1, keepdims=True))
        cots[...] = (cots[...].astype(F32) + dx).astype(BF)

    def backward(i, carry):
        l, place = n_layers - 1 - i // n_groups, lax.rem(i, n_groups)
        g = (n_layers * n_groups + i) * GROUP
        c0 = chunk_of(g)

        @pl.when(place == 0)
        def _():
            begin_backward(l)

        @pl.when(i >= RING // GROUP)
        def _():
            wait_group(g)

        bwd_down(l, g, c0, 0)
        bwd_down(l, g + 1, c0 + 1, 1)
        bwd_up(g, 0)

        @pl.when(g + RING < total)
        def _():
            dn_copy(g + RING).start()
            up_copy(g + RING).start()
            dn_copy(g + 1 + RING).start()

        bwd_down(l, g + 2, c0 + 2, 2)
        bwd_up(g + 1, 1)
        bwd_up(g + 2, 2)

        @pl.when(g + RING < total)
        def _():
            up_copy(g + 1 + RING).start()
            dn_copy(g + 2 + RING).start()
            up_copy(g + 2 + RING).start()

        @pl.when(place == n_groups - 1)
        def _():
            end_backward(l)

        return carry

    lax.fori_loop(0, (n_layers - 1) * n_groups, backward, 0)
    mixed_out[...] = dot(st[...], mixed_grad(0)).astype(BF).reshape(mixed_out.shape)
    send_blocks(n_emb, mixed_out, mixed_in, msem.at[0], msem.at[1])
    hand_over(1)
    hand_over(0)
    ids_to_partner.wait()
    write_out.wait()
    for l in reversed(range(n_layers)):
        to_hbm(l).wait()
        to_partner(l).wait()


def step(n_emb, tok_ids, resid, cot, tables, w_up, w_down, w_gate, w_proj, tf):
    t, d = resid.shape
    n_layers, n_rows, e = tables.shape
    f = w_up.shape[2]
    n_slots = n_emb * CAP
    vmem, hbm = pl.BlockSpec(memory_space=pltpu.VMEM), pl.BlockSpec(memory_space=pl.ANY)
    dma = pltpu.SemaphoreType.DMA
    return pl.pallas_call(
        functools.partial(step_kernel, n_layers, n_emb),
        out_shape=(jax.ShapeDtypeStruct((t, d), BF),
                   jax.ShapeDtypeStruct((2, n_layers, n_emb, CAP, e), F32),
                   jax.ShapeDtypeStruct((2, 8, 128), jnp.int32)),
        in_specs=[vmem] + [hbm] * 7,
        out_specs=(hbm, hbm, vmem),
        scratch_shapes=[
            pltpu.VMEM((RING, d, tf), BF),
            pltpu.VMEM((RING, tf, d), BF),
            pltpu.VMEM((n_layers, d, e), BF),
            pltpu.VMEM((n_layers, e, d), BF),
            pltpu.VMEM((2, f // tf, t, tf), F32),
            pltpu.VMEM((t, d), F32),
            pltpu.VMEM((n_layers, t, d), BF),
            pltpu.VMEM((t, d), BF),
            pltpu.VMEM((t, d), BF),
            pltpu.VMEM((GROUP, t, tf), BF),
            pltpu.VMEM((n_layers, t, e), F32),
            pltpu.VMEM((n_layers, t, e), F32),
            pltpu.VMEM((n_layers, t, e), BF),
            pltpu.VMEM((2, n_rows, e), BF),
            pltpu.VMEM((n_slots, t), BF),
            pltpu.VMEM((n_emb, 1, 128), jnp.int32),
            pltpu.VMEM((n_emb, 1, 128), jnp.int32),
            pltpu.VMEM((n_layers, n_emb, CAP, e), BF),
            pltpu.VMEM((n_layers, n_emb, CAP, e), BF),
            pltpu.VMEM((n_layers, n_emb, CAP, e), F32),
            pltpu.VMEM((n_layers, n_emb, CAP, e), F32),
            dma((4,)), dma((3 + n_layers,)), dma((n_layers,)), dma((2,)), dma((2,)),
            dma((2, n_layers)), dma((2, n_layers)), dma((2, n_layers)), dma((1 + n_layers,)), dma((2,)),
        ],
        compiler_params=pltpu.CompilerParams(collective_id=0, has_side_effects=True, vmem_limit_bytes=VMEM_LIMIT),
        name="step",
    )(tok_ids.reshape(1, t), resid, cot, tables, w_up, w_down, w_gate, w_proj)


def scatter_kernel(n_layers, n_rows, ids_ref, rows_hbm, x_hbm, out_hbm, x_out, rows, x, *scratch):
    acc, (insem, xsem, sem) = scratch[:n_layers], scratch[n_layers:]
    e = rows.shape[4]
    n_emb = rows.shape[2]
    loads = [pltpu.make_async_copy(rows_hbm.at[h], rows.at[h], insem.at[h]) for h in range(2)]
    x_in = pltpu.make_async_copy(x_hbm, x, xsem.at[0])
    x_back = pltpu.make_async_copy(x, x_out, xsem.at[1])
    for ld in loads + [x_in]:
        ld.start()

    def clear(i, carry):
        for l in range(n_layers):
            acc[l][pl.ds(pl.multiple_of(i * 64, 64), 64), :] = jnp.zeros((64, e), F32)
        return carry

    lax.fori_loop(0, n_rows // 64, clear, 0)
    per_row = min(128 // CAP, n_emb)

    for half in range(2):
        loads[half].wait()
        if half == 1:
            x_in.wait()
            x_back.start()
        for i in range(n_emb // per_row):
            def block(p, carry):
                b = i * per_row + p
                for k in range(0, CAP, 2):
                    v, w = ids_ref[half, i, p * CAP + k], ids_ref[half, i, p * CAP + k + 1]
                    same = v == w
                    for l in range(n_layers):
                        first, second = rows[half, l, b, k:k + 1, :], rows[half, l, b, k + 1:k + 2, :]
                        at_v, at_w = acc[l][pl.ds(v, 1), :], acc[l][pl.ds(w, 1), :]
                        acc[l][pl.ds(v, 1), :] = at_v + first
                        acc[l][pl.ds(w, 1), :] = at_w + (second + jnp.where(same, first, 0.0))
                return carry

            lax.fori_loop(0, per_row, block, 0)
    outs = [pltpu.make_async_copy(acc[l].at[pl.ds(0, n_rows)], out_hbm.at[l], sem.at[l]) for l in range(n_layers)]
    for cp in outs:
        cp.start()
    for cp in outs + [x_back]:
        cp.wait()


def scatter(ids, rows, x, n_rows):
    _, n_layers, n_emb, _, e = rows.shape
    hbm = pl.BlockSpec(memory_space=pl.ANY)
    return pl.pallas_call(
        functools.partial(scatter_kernel, n_layers, n_rows),
        out_shape=(jax.ShapeDtypeStruct((n_layers, n_rows, e), F32), jax.ShapeDtypeStruct(x.shape, x.dtype)),
        in_specs=[pl.BlockSpec(memory_space=pltpu.SMEM), hbm, hbm],
        out_specs=(hbm, hbm),
        scratch_shapes=[pltpu.VMEM(rows.shape, F32), pltpu.VMEM(x.shape, x.dtype)]
        + [pltpu.VMEM((n_rows + 8, e), F32)] * n_layers
        + [pltpu.SemaphoreType.DMA((2,)), pltpu.SemaphoreType.DMA((2,)), pltpu.SemaphoreType.DMA((n_layers,))],
        compiler_params=pltpu.CompilerParams(vmem_limit_bytes=VMEM_LIMIT),
        name="scatter",
    )(ids, rows, x)


def solution(mesh):
    n_emb = mesh.shape["emb"]
    tok_spec = P(("dp", "emb"))
    act_spec = P(("dp", "emb"), None)
    table_spec = P(None, "emb", None)
    full_spec = P(None, None, None)

    def device_body(tok_ids, resid_in, cot_out, tables, w_up, w_down, w_gate, w_proj):
        f = w_up.shape[2]
        tf = 768 if f % (9 * 768) == 0 else 256
        resid_out, rows, ids = step(n_emb, tok_ids, resid_in, cot_out, tables, w_up, w_down, w_gate, w_proj, tf)
        d_tables, resid_out = scatter(ids, rows, resid_out, tables.shape[1])
        return resid_out, d_tables

    return jax.shard_map(device_body, mesh=mesh,
                         in_specs=(tok_spec, act_spec, act_spec, table_spec, full_spec, full_spec, full_spec, full_spec),
                         out_specs=(act_spec, table_spec), check_vma=False)
```

```python
import functools
import math

import jax
import jax.numpy as jnp
from jax import lax
from jax.experimental import pallas as pl
from jax.experimental.pallas import tpu as pltpu
from jax.sharding import PartitionSpec as P

NORM_EPS = 1e-6
CAP = 8
BF = jnp.bfloat16
F32 = jnp.float32
MESH_ID = pl.DeviceIdType.MESH
VMEM_LIMIT = 67_043_328
GELU_C = math.sqrt(2.0 / math.pi)


def dot(a, b):
    return jnp.dot(a, b, preferred_element_type=F32)


def dot_nt(a, b):
    return lax.dot_general(a, b, (((1,), (1,)), ((), ())), preferred_element_type=F32)


def dot_tn(a, b):
    return lax.dot_general(a, b, (((0,), (0,)), ((), ())), preferred_element_type=F32)


def iota(shape, axis):
    return lax.broadcasted_iota(jnp.int32, shape, axis)


def gelu_both(x):
    x2 = x * x
    t = jnp.tanh(x * (GELU_C + (GELU_C * 0.044715) * x2))
    hx = 0.5 * x
    s = 0.5 + 0.5 * t
    d = s + hx * (1.0 - t * t) * (GELU_C + (3.0 * GELU_C * 0.044715) * x2)
    return x * s, d


def inv_rms(x):
    return lax.rsqrt(jnp.mean(x * x, axis=-1, keepdims=True) + NORM_EPS)


def peers_barrier(n_emb):
    me, dp = lax.axis_index("emb"), lax.axis_index("dp")
    bar = pltpu.get_barrier_semaphore()

    def tell(k, carry):
        pl.semaphore_signal(bar, inc=1, device_id={"emb": lax.rem(me + k, n_emb)}, device_id_type=MESH_ID)
        return carry

    lax.fori_loop(1, n_emb, tell, 0)
    pl.semaphore_signal(bar, inc=1, device_id={"dp": 1 - dp}, device_id_type=MESH_ID)
    return bar


def send_blocks(n_emb, src, dst, send_sem, recv_sem):
    me = lax.axis_index("emb")

    def one(k, carry):
        to = lax.rem(me + k, n_emb)
        pltpu.make_async_remote_copy(
            src_ref=src.at[to], dst_ref=dst.at[me], send_sem=send_sem, recv_sem=recv_sem,
            device_id={"emb": to}, device_id_type=MESH_ID).start()
        return carry

    lax.fori_loop(1, n_emb, one, 0)


def blocks_desc(n_emb, src, dst, send_sem, recv_sem):
    me = lax.axis_index("emb")
    return pltpu.make_async_remote_copy(
        src_ref=src.at[pl.ds(0, n_emb - 1)], dst_ref=dst.at[pl.ds(0, n_emb - 1)],
        send_sem=send_sem, recv_sem=recv_sem, device_id={"emb": me}, device_id_type=MESH_ID)


def partner_copy(src, dst, send_sem, recv_sem):
    return pltpu.make_async_remote_copy(
        src_ref=src, dst_ref=dst, send_sem=send_sem, recv_sem=recv_sem,
        device_id={"dp": 1 - lax.axis_index("dp")}, device_id_type=MESH_ID)


RING = 6
GROUP = 3


def step_kernel(n_layers, n_emb, ids_ref, resid_hbm, cot_hbm, table_hbm, up_hbm, down_hbm, gate_hbm, proj_hbm,
                out_hbm, rows_hbm, rid_ref,
                wup, wdn, gate, proj, gp, acc, xs, us, cots, hid, gval, gder, fetched,
                table, st, sid, rid, served, fetch_in, grad_out, grad_in,
                ringsem, ldsem, tsem, isem, psem, fsem, gsem, dsem, wsem, msem):
    me = lax.axis_index("emb")
    n_rows, e = table.shape[1:]
    t_chunk = min(1024, n_rows)
    t, d = acc.shape
    tf = wup.shape[2]
    n_slots = n_emb * CAP
    n_chunks = up_hbm.shape[2] // tf
    n_groups = n_chunks // GROUP
    total = (2 * n_layers - 1) * n_chunks

    def layer_of(g):
        if isinstance(g, int):
            return 0
        p = g // n_chunks
        return jnp.minimum(p, 2 * n_layers - 1 - p)

    def chunk_of(g):
        if isinstance(g, int):
            return g
        turn = jnp.where(g // n_chunks == n_layers, n_chunks - RING, 0)
        return lax.rem(g + turn, n_chunks)

    def slot_of(g):
        return g % RING if isinstance(g, int) else lax.rem(g, RING)

    def up_copy(g):
        c, s = chunk_of(g), slot_of(g)
        return pltpu.make_async_copy(up_hbm.at[layer_of(g), :, pl.ds(c * tf if isinstance(c, int) else pl.multiple_of(c * tf, tf), tf)],
                                     wup.at[s], ringsem.at[0, s])

    def dn_copy(g):
        c, s = chunk_of(g), slot_of(g)
        return pltpu.make_async_copy(down_hbm.at[layer_of(g), pl.ds(c * tf if isinstance(c, int) else pl.multiple_of(c * tf, tf), tf), :],
                                     wdn.at[s], ringsem.at[1, s])

    load_x = pltpu.make_async_copy(resid_hbm, xs.at[0], ldsem.at[0])
    load_cot = pltpu.make_async_copy(cot_hbm, cots, ldsem.at[1])
    load_proj = pltpu.make_async_copy(proj_hbm, proj, ldsem.at[2])
    load_gate = [pltpu.make_async_copy(gate_hbm.at[l], gate.at[l], ldsem.at[3 + l]) for l in range(n_layers)]
    load_table = [pltpu.make_async_copy(table_hbm.at[l], table.at[l % 2], tsem.at[l]) for l in range(min(n_layers, 2))]
    load_x.start()
    load_gate[0].start()
    for g in range(RING):
        up_copy(g).start()
        dn_copy(g).start()
    for ld in load_table + [load_proj] + load_gate[1:] + [load_cot]:
        ld.start()
    bar = peers_barrier(n_emb)


    ids = ids_ref[...]
    shift = n_rows.bit_length() - 1
    owner = lax.shift_right_logical(ids, shift)
    local = ids - lax.shift_left(owner, shift) + 1
    own_t = owner == iota((n_emb, t), 0)
    before = (iota((t, t), 0) < iota((t, t), 1)).astype(F32).astype(BF)
    own_f = own_t.astype(F32)
    rank = jnp.sum(own_f * dot(own_f.astype(BF), before), axis=0, keepdims=True).astype(jnp.int32)
    st[...] = (owner * CAP + rank == iota((n_slots, t), 0)).astype(F32).astype(BF)
    rank_t = (rank == iota((128, t), 0)).astype(F32).astype(BF)
    id_hi = jnp.where(own_t, lax.shift_right_logical(local, 6).astype(F32), 0.0).astype(BF)
    id_lo = jnp.where(own_t, jnp.bitwise_and(local, 63).astype(F32), 0.0).astype(BF)
    sid[...] = (64.0 * dot_nt(id_hi, rank_t) + dot_nt(id_lo, rank_t)).astype(jnp.int32).reshape(sid.shape)

    def send_ids():
        pl.semaphore_wait(bar, n_emb)
        send_blocks(n_emb, sid, rid, isem.at[0], isem.at[1])

    ids_to_partner = partner_copy(rid_ref.at[0], rid_ref.at[1], psem.at[0], psem.at[1])

    def serve():
        blocks_desc(n_emb, sid, rid, isem.at[0], isem.at[1]).wait()
        rid[me] = sid[me]
        ids_in = rid[...].reshape(n_emb, 128)
        spread = (lax.shift_right_logical(iota((n_slots, n_emb), 0), 3) == iota((n_slots, n_emb), 1))
        spread = spread.astype(F32).astype(BF)
        hi = lax.shift_right_logical(ids_in, 6).astype(F32).astype(BF)
        lo = jnp.bitwise_and(ids_in, 63).astype(F32).astype(BF)
        pick = jnp.bitwise_and(iota((n_slots, 128), 0), CAP - 1) == iota((n_slots, 128), 1)
        col_hi = jnp.sum(jnp.where(pick, dot(spread, hi), 0.0), axis=1, keepdims=True)
        col_lo = jnp.sum(jnp.where(pick, dot(spread, lo), 0.0), axis=1, keepdims=True)
        col = (64.0 * col_hi + col_lo).astype(jnp.int32) - 1
        chunk = t_chunk
        for l in range(n_layers):
            pltpu.make_async_copy(table_hbm.at[l], table.at[l % 2], tsem.at[l]).wait()
            sel = None
            for c in range(n_rows // chunk):
                oh = (col == iota((n_slots, chunk), 1) + c * chunk).astype(F32).astype(BF)
                part = dot(oh, table[l % 2, c * chunk:(c + 1) * chunk, :])
                if l + 2 < n_layers:
                    piece = pl.ds(c * chunk, chunk)
                    pltpu.make_async_copy(table_hbm.at[l + 2, piece], table.at[l % 2, piece], tsem.at[l + 2]).start()
                sel = part if sel is None else sel + part
            served[l] = sel.astype(BF).reshape(n_emb, CAP, e)
            send_blocks(n_emb, served.at[l], fetch_in.at[l], fsem.at[0, l], fsem.at[1, l])
        lane = jnp.bitwise_and(iota((n_slots, 128), 0), 127) == iota((n_slots, 128), 1)
        row = (lax.shift_right_logical(iota((8, n_slots), 1), 7) == iota((8, n_slots), 0)).astype(F32).astype(BF)
        flat_hi = dot(row, jnp.where(lane, col_hi, 0.0).astype(BF))
        flat_lo = dot(row, jnp.where(lane, col_lo, 0.0).astype(BF))
        flat = (64.0 * flat_hi + flat_lo).astype(jnp.int32) - 1
        spare = n_rows + jnp.bitwise_and(iota(flat.shape, 1), 1)
        rid_ref[0] = jnp.where(flat < 0, spare, flat)
        ids_to_partner.start()

    def send_rows(l, rows):
        hi = rows.astype(BF)
        rest = rows - hi.astype(F32)
        mid = rest.astype(BF)
        low = (rest - mid.astype(F32)).astype(BF)
        slots = dot(st[...], hi) + dot(st[...], mid) + dot(st[...], low)
        grad_out[l] = slots.reshape(grad_out.shape[1:])
        send_blocks(n_emb, grad_out.at[l], grad_in.at[l], gsem.at[0, l], gsem.at[1, l])


    def begin_forward(l):
        x = xs[l].astype(F32)
        us[...] = (x * inv_rms(x)).astype(BF)
        g, der = gelu_both(dot(us[...], gate[l]))
        gval[l] = g
        gder[l] = der
        acc[...] = x

    n_sub = tf // 256

    def fwd_up(l, g, c, k, more):
        w = wup.at[lax.rem(g, RING)]
        for j in range(n_sub):
            cols = slice(j * 256, (j + 1) * 256)
            h, der = gelu_both(dot(us[...], w[:, cols]))
            hid[k, :, cols] = h.astype(BF)
            gp[lax.rem(l + 1, 2), c, :, cols] = der
        if more:
            up_copy(g + RING).start()

    def fwd_down(g, k, more):
        acc[...] += dot(hid[k], wdn[lax.rem(g, RING)])
        if more:
            dn_copy(g + RING).start()

    def wait_group(g, first=0, n=GROUP):
        for k in range(first, first + n):
            up_copy(g + k).wait()
            dn_copy(g + k).wait()

    def end_forward(l):
        for q in range(n_layers):
            @pl.when(l == q)
            def _():
                blocks_desc(n_emb, served.at[q], fetch_in.at[q], fsem.at[0, q], fsem.at[1, q]).wait()
        @pl.when(l == 0)
        def _():
            for ld in [load_proj] + load_gate[1:]:
                ld.wait()

        fetch_in[l, me] = served[l, me]
        fetched[l] = dot_tn(st[...], fetch_in[l].reshape(n_slots, e)).astype(BF)
        mixed = (gval[l] * fetched[l].astype(F32)).astype(BF)
        xs[lax.rem(l + 1, n_layers)] = (acc[...] + dot(mixed, proj[l])).astype(BF)

    def forward(more, i, carry):
        l, c0 = i // n_groups, lax.rem(i, n_groups) * GROUP
        g = i * GROUP

        if more:
            @pl.when(c0 == 0)
            def _():
                begin_forward(l)

            @pl.when(i == 2)
            def _():
                serve()

        wait_group(g)
        fwd_up(l, g, c0, 0, more)
        fwd_up(l, g + 1, c0 + 1, 1, more)
        fwd_down(g, 0, more)
        fwd_up(l, g + 2, c0 + 2, 2, more)
        fwd_down(g + 1, 1, more)
        fwd_down(g + 2, 2, more)

        @pl.when(c0 == n_chunks - GROUP)
        def _():
            end_forward(l)

        return carry

    load_x.wait()
    load_gate[0].wait()
    begin_forward(0)
    wait_group(0, 0, 1)
    fwd_up(0, jnp.int32(0), 0, 0, True)
    fwd_down(jnp.int32(0), 0, True)
    wait_group(0, 1, GROUP - 1)
    for k in range(1, GROUP):
        fwd_up(0, jnp.int32(k), k, k, True)
    for k in range(1, GROUP):
        fwd_down(jnp.int32(k), k, True)
    send_ids()
    kept = n_layers * n_groups - RING // GROUP
    lax.fori_loop(1, kept, functools.partial(forward, True), 0)
    lax.fori_loop(kept, n_layers * n_groups, functools.partial(forward, False), 0)
    write_out = pltpu.make_async_copy(xs.at[0], out_hbm, wsem.at[0])
    write_out.start()
    load_cot.wait()
    send_rows(0, gval[0])


    def mixed_grad(l):
        return dot_nt(cots[...], proj[l]).astype(BF)

    def send_grads(l):
        d_mixed = mixed_grad(l).astype(F32)
        send_rows(l, gval[l] * d_mixed)
        return d_mixed

    mixed_out, mixed_in = served.at[0], fetch_in.at[0]

    def to_partner(l):
        return partner_copy(grad_in.at[l], rows_hbm.at[1, l], dsem.at[0, l], dsem.at[1, l])

    def to_hbm(l):
        return pltpu.make_async_copy(grad_in.at[l], rows_hbm.at[0, l], wsem.at[1 + l])

    def mixed_desc():
        return blocks_desc(n_emb, mixed_out, mixed_in, msem.at[0], msem.at[1])

    def hand_over(l):
        blocks_desc(n_emb, grad_out.at[l], grad_in.at[l], gsem.at[0, l], gsem.at[1, l]).wait()
        grad_in[l, me] = grad_out[l, me]
        if l == 0:
            mixed_desc().wait()
            mixed_in[me] = mixed_out[me]
            grad_in[0] = grad_in[0] * mixed_in[...].astype(F32)
        to_partner(l).start()
        to_hbm(l).start()

    def begin_backward(l):
        d_mixed = send_grads(l)
        for q in range(2, n_layers):
            @pl.when(l == q - 1)
            def _():
                hand_over(q)

        d_gate = (gder[l] * (d_mixed * fetched[l].astype(F32))).astype(BF)
        us[...] = dot_nt(d_gate, gate[l]).astype(BF)
        acc[...] = jnp.zeros_like(acc)

    def bwd_down(l, g, c, k):
        w = wdn.at[lax.rem(g, RING)]
        for j in range(n_sub):
            cols = slice(j * 256, (j + 1) * 256)
            dh = dot_nt(cots[...], w[cols, :]).astype(BF).astype(F32)
            hid[k, :, cols] = (gp[lax.rem(l + 1, 2), c, :, cols] * dh).astype(BF)

    def bwd_up(g, k):
        acc[...] += dot_nt(hid[k], wup[lax.rem(g, RING)])

    def end_backward(l):
        d_norm = (acc[...].astype(BF).astype(F32) + us[...].astype(F32)).astype(BF).astype(F32)
        x = xs[l].astype(F32)
        r = inv_rms(x)
        dx = r * d_norm - x * (r * r * r * jnp.mean(x * d_norm, axis=-1, keepdims=True))
        cots[...] = (cots[...].astype(F32) + dx).astype(BF)

    def backward(i, carry):
        l, place = n_layers - 1 - i // n_groups, lax.rem(i, n_groups)
        g = (n_layers * n_groups + i) * GROUP
        c0 = chunk_of(g)

        @pl.when(place == 0)
        def _():
            begin_backward(l)

        @pl.when(i >= RING // GROUP)
        def _():
            wait_group(g)

        bwd_down(l, g, c0, 0)
        bwd_down(l, g + 1, c0 + 1, 1)
        bwd_up(g, 0)

        @pl.when(g + RING < total)
        def _():
            dn_copy(g + RING).start()
            up_copy(g + RING).start()
            dn_copy(g + 1 + RING).start()

        bwd_down(l, g + 2, c0 + 2, 2)
        bwd_up(g + 1, 1)
        bwd_up(g + 2, 2)

        @pl.when(g + RING < total)
        def _():
            up_copy(g + 1 + RING).start()
            dn_copy(g + 2 + RING).start()
            up_copy(g + 2 + RING).start()

        @pl.when(place == n_groups - 1)
        def _():
            end_backward(l)

        return carry

    lax.fori_loop(0, (n_layers - 1) * n_groups, backward, 0)
    mixed_out[...] = dot(st[...], mixed_grad(0)).astype(BF).reshape(mixed_out.shape)
    send_blocks(n_emb, mixed_out, mixed_in, msem.at[0], msem.at[1])
    hand_over(1)
    hand_over(0)
    ids_to_partner.wait()
    write_out.wait()
    for l in reversed(range(n_layers)):
        to_hbm(l).wait()
        to_partner(l).wait()


def step(n_emb, tok_ids, resid, cot, tables, w_up, w_down, w_gate, w_proj, tf):
    t, d = resid.shape
    n_layers, n_rows, e = tables.shape
    f = w_up.shape[2]
    n_slots = n_emb * CAP
    vmem, hbm = pl.BlockSpec(memory_space=pltpu.VMEM), pl.BlockSpec(memory_space=pl.ANY)
    dma = pltpu.SemaphoreType.DMA
    return pl.pallas_call(
        functools.partial(step_kernel, n_layers, n_emb),
        out_shape=(jax.ShapeDtypeStruct((t, d), BF),
                   jax.ShapeDtypeStruct((2, n_layers, n_emb, CAP, e), F32),
                   jax.ShapeDtypeStruct((2, 8, 128), jnp.int32)),
        in_specs=[vmem] + [hbm] * 7,
        out_specs=(hbm, hbm, vmem),
        scratch_shapes=[
            pltpu.VMEM((RING, d, tf), BF),
            pltpu.VMEM((RING, tf, d), BF),
            pltpu.VMEM((n_layers, d, e), BF),
            pltpu.VMEM((n_layers, e, d), BF),
            pltpu.VMEM((2, f // tf, t, tf), F32),
            pltpu.VMEM((t, d), F32),
            pltpu.VMEM((n_layers, t, d), BF),
            pltpu.VMEM((t, d), BF),
            pltpu.VMEM((t, d), BF),
            pltpu.VMEM((GROUP, t, tf), BF),
            pltpu.VMEM((n_layers, t, e), F32),
            pltpu.VMEM((n_layers, t, e), F32),
            pltpu.VMEM((n_layers, t, e), BF),
            pltpu.VMEM((2, n_rows, e), BF),
            pltpu.VMEM((n_slots, t), BF),
            pltpu.VMEM((n_emb, 1, 128), jnp.int32),
            pltpu.VMEM((n_emb, 1, 128), jnp.int32),
            pltpu.VMEM((n_layers, n_emb, CAP, e), BF),
            pltpu.VMEM((n_layers, n_emb, CAP, e), BF),
            pltpu.VMEM((n_layers, n_emb, CAP, e), F32),
            pltpu.VMEM((n_layers, n_emb, CAP, e), F32),
            dma((2, RING)), dma((3 + n_layers,)), dma((n_layers,)), dma((2,)), dma((2,)),
            dma((2, n_layers)), dma((2, n_layers)), dma((2, n_layers)), dma((1 + n_layers,)), dma((2,)),
        ],
        compiler_params=pltpu.CompilerParams(collective_id=0, has_side_effects=True, vmem_limit_bytes=VMEM_LIMIT),
        name="step",
    )(tok_ids.reshape(1, t), resid, cot, tables, w_up, w_down, w_gate, w_proj)


def scatter_kernel(n_layers, n_rows, ids_ref, rows_hbm, x_hbm, out_hbm, x_out, rows, x, *scratch):
    acc, (insem, xsem, sem) = scratch[:n_layers], scratch[n_layers:]
    e = rows.shape[4]
    n_emb = rows.shape[2]
    loads = [pltpu.make_async_copy(rows_hbm.at[h], rows.at[h], insem.at[h]) for h in range(2)]
    x_in = pltpu.make_async_copy(x_hbm, x, xsem.at[0])
    x_back = pltpu.make_async_copy(x, x_out, xsem.at[1])
    for ld in loads + [x_in]:
        ld.start()

    def clear(i, carry):
        for l in range(n_layers):
            acc[l][pl.ds(pl.multiple_of(i * 64, 64), 64), :] = jnp.zeros((64, e), F32)
        return carry

    lax.fori_loop(0, n_rows // 64, clear, 0)
    per_row = min(128 // CAP, n_emb)

    for half in range(2):
        loads[half].wait()
        if half == 1:
            x_in.wait()
            x_back.start()
        for i in range(n_emb // per_row):
            def block(p, carry):
                b = i * per_row + p

                def pairs(k0, k1):
                    for k in range(k0, k1, 2):
                        v, w = ids_ref[half, i, p * CAP + k], ids_ref[half, i, p * CAP + k + 1]
                        same = v == w
                        for l in range(n_layers):
                            first, second = rows[half, l, b, k:k + 1, :], rows[half, l, b, k + 1:k + 2, :]
                            at_v, at_w = acc[l][pl.ds(v, 1), :], acc[l][pl.ds(w, 1), :]
                            acc[l][pl.ds(v, 1), :] = at_v + first
                            acc[l][pl.ds(w, 1), :] = at_w + (second + jnp.where(same, first, 0.0))

                pairs(0, CAP // 2)

                @pl.when(ids_ref[half, i, p * CAP + CAP // 2] < n_rows)
                def _():
                    pairs(CAP // 2, CAP)

                return carry

            lax.fori_loop(0, per_row, block, 0)
    outs = [pltpu.make_async_copy(acc[l].at[pl.ds(0, n_rows)], out_hbm.at[l], sem.at[l]) for l in range(n_layers)]
    for cp in outs:
        cp.start()
    for cp in outs + [x_back]:
        cp.wait()


def scatter(ids, rows, x, n_rows):
    _, n_layers, n_emb, _, e = rows.shape
    hbm = pl.BlockSpec(memory_space=pl.ANY)
    return pl.pallas_call(
        functools.partial(scatter_kernel, n_layers, n_rows),
        out_shape=(jax.ShapeDtypeStruct((n_layers, n_rows, e), F32), jax.ShapeDtypeStruct(x.shape, x.dtype)),
        in_specs=[pl.BlockSpec(memory_space=pltpu.SMEM), hbm, hbm],
        out_specs=(hbm, hbm),
        scratch_shapes=[pltpu.VMEM(rows.shape, F32), pltpu.VMEM(x.shape, x.dtype)]
        + [pltpu.VMEM((n_rows + 8, e), F32)] * n_layers
        + [pltpu.SemaphoreType.DMA((2,)), pltpu.SemaphoreType.DMA((2,)), pltpu.SemaphoreType.DMA((n_layers,))],
        compiler_params=pltpu.CompilerParams(vmem_limit_bytes=VMEM_LIMIT),
        name="scatter",
    )(ids, rows, x)


def solution(mesh):
    n_emb = mesh.shape["emb"]
    tok_spec = P(("dp", "emb"))
    act_spec = P(("dp", "emb"), None)
    table_spec = P(None, "emb", None)
    full_spec = P(None, None, None)

    def device_body(tok_ids, resid_in, cot_out, tables, w_up, w_down, w_gate, w_proj):
        f = w_up.shape[2]
        tf = 768 if f % (9 * 768) == 0 else 256
        resid_out, rows, ids = step(n_emb, tok_ids, resid_in, cot_out, tables, w_up, w_down, w_gate, w_proj, tf)
        d_tables, resid_out = scatter(ids, rows, resid_out, tables.shape[1])
        return resid_out, d_tables

    return jax.shard_map(device_body, mesh=mesh,
                         in_specs=(tok_spec, act_spec, act_spec, table_spec, full_spec, full_spec, full_spec, full_spec),
                         out_specs=(act_spec, table_spec), check_vma=False)
```

```python
import functools
import math

import jax
import jax.numpy as jnp
from jax import lax
from jax.experimental import pallas as pl
from jax.experimental.pallas import tpu as pltpu
from jax.sharding import PartitionSpec as P

NORM_EPS = 1e-6
CAP = 8
BF = jnp.bfloat16
F32 = jnp.float32
MESH_ID = pl.DeviceIdType.MESH
VMEM_LIMIT = 67_043_328
GELU_C = math.sqrt(2.0 / math.pi)


def dot(a, b):
    return jnp.dot(a, b, preferred_element_type=F32)


def dot_nt(a, b):
    return lax.dot_general(a, b, (((1,), (1,)), ((), ())), preferred_element_type=F32)


def dot_tn(a, b):
    return lax.dot_general(a, b, (((0,), (0,)), ((), ())), preferred_element_type=F32)


def iota(shape, axis):
    return lax.broadcasted_iota(jnp.int32, shape, axis)


def gelu_both(x):
    x2 = x * x
    t = jnp.tanh(x * (GELU_C + (GELU_C * 0.044715) * x2))
    hx = 0.5 * x
    s = 0.5 + 0.5 * t
    d = s + hx * (1.0 - t * t) * (GELU_C + (3.0 * GELU_C * 0.044715) * x2)
    return x * s, d


def inv_rms(x):
    return lax.rsqrt(jnp.mean(x * x, axis=-1, keepdims=True) + NORM_EPS)


def peers_barrier(n_emb):
    me, dp = lax.axis_index("emb"), lax.axis_index("dp")
    bar = pltpu.get_barrier_semaphore()

    def tell(k, carry):
        pl.semaphore_signal(bar, inc=1, device_id={"emb": lax.rem(me + k, n_emb)}, device_id_type=MESH_ID)
        return carry

    lax.fori_loop(1, n_emb, tell, 0)
    pl.semaphore_signal(bar, inc=1, device_id={"dp": 1 - dp}, device_id_type=MESH_ID)
    return bar


def send_blocks(n_emb, src, dst, send_sem, recv_sem):
    me = lax.axis_index("emb")

    def one(k, carry):
        to = lax.rem(me + k, n_emb)
        pltpu.make_async_remote_copy(
            src_ref=src.at[to], dst_ref=dst.at[me], send_sem=send_sem, recv_sem=recv_sem,
            device_id={"emb": to}, device_id_type=MESH_ID).start()
        return carry

    lax.fori_loop(1, n_emb, one, 0)


def blocks_desc(n_emb, src, dst, send_sem, recv_sem):
    me = lax.axis_index("emb")
    return pltpu.make_async_remote_copy(
        src_ref=src.at[pl.ds(0, n_emb - 1)], dst_ref=dst.at[pl.ds(0, n_emb - 1)],
        send_sem=send_sem, recv_sem=recv_sem, device_id={"emb": me}, device_id_type=MESH_ID)


def partner_copy(src, dst, send_sem, recv_sem):
    return pltpu.make_async_remote_copy(
        src_ref=src, dst_ref=dst, send_sem=send_sem, recv_sem=recv_sem,
        device_id={"dp": 1 - lax.axis_index("dp")}, device_id_type=MESH_ID)


RING = 6
GROUP = 3


def step_kernel(n_layers, n_emb, ids_ref, resid_hbm, cot_hbm, table_hbm, up_hbm, down_hbm, gate_hbm, proj_hbm,
                out_hbm, rows_hbm, rid_ref,
                wup, wdn, gate, proj, gp, acc, xs, us, cots, hid, gval, gder, fetched,
                table, st, sid, rid, served, fetch_in, grad_out, grad_in,
                ringsem, ldsem, tsem, isem, psem, fsem, gsem, dsem, wsem, msem):
    me = lax.axis_index("emb")
    n_rows, e = table.shape[1:]
    t_chunk = min(1024, n_rows)
    t, d = acc.shape
    tf = wup.shape[2]
    n_slots = n_emb * CAP
    n_chunks = up_hbm.shape[2] // tf
    n_groups = n_chunks // GROUP
    total = (2 * n_layers - 1) * n_chunks

    def layer_of(g):
        if isinstance(g, int):
            return 0
        p = g // n_chunks
        return jnp.minimum(p, 2 * n_layers - 1 - p)

    def chunk_of(g):
        if isinstance(g, int):
            return g
        turn = jnp.where(g // n_chunks == n_layers, n_chunks - RING, 0)
        return lax.rem(g + turn, n_chunks)

    def slot_of(g):
        return g % RING if isinstance(g, int) else lax.rem(g, RING)

    def up_copy(g):
        c, s = chunk_of(g), slot_of(g)
        return pltpu.make_async_copy(up_hbm.at[layer_of(g), :, pl.ds(c * tf if isinstance(c, int) else pl.multiple_of(c * tf, tf), tf)],
                                     wup.at[s], ringsem.at[0, s])

    def dn_copy(g):
        c, s = chunk_of(g), slot_of(g)
        return pltpu.make_async_copy(down_hbm.at[layer_of(g), pl.ds(c * tf if isinstance(c, int) else pl.multiple_of(c * tf, tf), tf), :],
                                     wdn.at[s], ringsem.at[1, s])

    load_x = pltpu.make_async_copy(resid_hbm, xs.at[0], ldsem.at[0])
    load_cot = pltpu.make_async_copy(cot_hbm, cots, ldsem.at[1])
    load_proj = pltpu.make_async_copy(proj_hbm, proj, ldsem.at[2])
    load_gate = [pltpu.make_async_copy(gate_hbm.at[l], gate.at[l], ldsem.at[3 + l]) for l in range(n_layers)]
    load_table = [pltpu.make_async_copy(table_hbm.at[l], table.at[l], tsem.at[l]) for l in range(n_layers)]
    load_x.start()
    load_gate[0].start()
    for g in range(RING):
        up_copy(g).start()
        dn_copy(g).start()
    for ld in load_table + [load_proj] + load_gate[1:] + [load_cot]:
        ld.start()
    bar = peers_barrier(n_emb)


    ids = ids_ref[...]
    shift = n_rows.bit_length() - 1
    owner = lax.shift_right_logical(ids, shift)
    local = ids - lax.shift_left(owner, shift) + 1
    own_t = owner == iota((n_emb, t), 0)
    before = (iota((t, t), 0) < iota((t, t), 1)).astype(F32).astype(BF)
    own_f = own_t.astype(F32)
    rank = jnp.sum(own_f * dot(own_f.astype(BF), before), axis=0, keepdims=True).astype(jnp.int32)
    st[...] = (owner * CAP + rank == iota((n_slots, t), 0)).astype(F32).astype(BF)
    rank_t = (rank == iota((128, t), 0)).astype(F32).astype(BF)
    id_hi = jnp.where(own_t, lax.shift_right_logical(local, 6).astype(F32), 0.0).astype(BF)
    id_lo = jnp.where(own_t, jnp.bitwise_and(local, 63).astype(F32), 0.0).astype(BF)
    sid[...] = (64.0 * dot_nt(id_hi, rank_t) + dot_nt(id_lo, rank_t)).astype(jnp.int32).reshape(sid.shape)

    def send_ids():
        pl.semaphore_wait(bar, n_emb)
        send_blocks(n_emb, sid, rid, isem.at[0], isem.at[1])

    ids_to_partner = partner_copy(rid_ref.at[0], rid_ref.at[1], psem.at[0], psem.at[1])

    def serve():
        blocks_desc(n_emb, sid, rid, isem.at[0], isem.at[1]).wait()
        rid[me] = sid[me]
        ids_in = rid[...].reshape(n_emb, 128)
        spread = (lax.shift_right_logical(iota((n_slots, n_emb), 0), 3) == iota((n_slots, n_emb), 1))
        spread = spread.astype(F32).astype(BF)
        hi = lax.shift_right_logical(ids_in, 6).astype(F32).astype(BF)
        lo = jnp.bitwise_and(ids_in, 63).astype(F32).astype(BF)
        pick = jnp.bitwise_and(iota((n_slots, 128), 0), CAP - 1) == iota((n_slots, 128), 1)
        col_hi = jnp.sum(jnp.where(pick, dot(spread, hi), 0.0), axis=1, keepdims=True)
        col_lo = jnp.sum(jnp.where(pick, dot(spread, lo), 0.0), axis=1, keepdims=True)
        col = (64.0 * col_hi + col_lo).astype(jnp.int32) - 1
        for l in range(n_layers):
            load_table[l].wait()

            def piece(c, sel):
                oh = (col == iota((n_slots, t_chunk), 1) + c * t_chunk).astype(F32).astype(BF)
                return sel + dot(oh, table[l, pl.ds(pl.multiple_of(c * t_chunk, t_chunk), t_chunk), :])

            sel = lax.fori_loop(0, n_rows // t_chunk, piece, jnp.zeros((n_slots, e), F32))
            served[l] = sel.astype(BF).reshape(n_emb, CAP, e)
            send_blocks(n_emb, served.at[l], fetch_in.at[l], fsem.at[0, l], fsem.at[1, l])
        lane = jnp.bitwise_and(iota((n_slots, 128), 0), 127) == iota((n_slots, 128), 1)
        row = (lax.shift_right_logical(iota((8, n_slots), 1), 7) == iota((8, n_slots), 0)).astype(F32).astype(BF)
        flat_hi = dot(row, jnp.where(lane, col_hi, 0.0).astype(BF))
        flat_lo = dot(row, jnp.where(lane, col_lo, 0.0).astype(BF))
        flat = (64.0 * flat_hi + flat_lo).astype(jnp.int32) - 1
        spare = n_rows + jnp.bitwise_and(iota(flat.shape, 1), 1)
        rid_ref[0] = jnp.where(flat < 0, spare, flat)
        ids_to_partner.start()

    def send_rows(l, rows):
        hi = rows.astype(BF)
        rest = rows - hi.astype(F32)
        mid = rest.astype(BF)
        low = (rest - mid.astype(F32)).astype(BF)
        slots = dot(st[...], hi) + dot(st[...], mid) + dot(st[...], low)
        grad_out[l] = slots.reshape(grad_out.shape[1:])
        send_blocks(n_emb, grad_out.at[l], grad_in.at[l], gsem.at[0, l], gsem.at[1, l])


    def begin_forward(l):
        x = xs[l].astype(F32)
        us[...] = (x * inv_rms(x)).astype(BF)
        g, der = gelu_both(dot(us[...], gate[l]))
        gval[l] = g
        gder[l] = der
        acc[...] = x

    n_sub = tf // 256

    def fwd_up(l, g, c, k, more):
        w = wup.at[lax.rem(g, RING)]
        for j in range(n_sub):
            cols = slice(j * 256, (j + 1) * 256)
            h, der = gelu_both(dot(us[...], w[:, cols]))
            hid[k, :, cols] = h.astype(BF)
            gp[lax.rem(l + 1, 2), c, :, cols] = der
        if more:
            up_copy(g + RING).start()

    def fwd_down(g, k, more):
        acc[...] += dot(hid[k], wdn[lax.rem(g, RING)])
        if more:
            dn_copy(g + RING).start()

    def wait_group(g, first=0, n=GROUP):
        for k in range(first, first + n):
            up_copy(g + k).wait()
            dn_copy(g + k).wait()

    def end_forward(l):
        for q in range(n_layers):
            @pl.when(l == q)
            def _():
                blocks_desc(n_emb, served.at[q], fetch_in.at[q], fsem.at[0, q], fsem.at[1, q]).wait()
        @pl.when(l == 0)
        def _():
            for ld in [load_proj] + load_gate[1:]:
                ld.wait()

        fetch_in[l, me] = served[l, me]
        fetched[l] = dot_tn(st[...], fetch_in[l].reshape(n_slots, e)).astype(BF)
        mixed = (gval[l] * fetched[l].astype(F32)).astype(BF)
        xs[lax.rem(l + 1, n_layers)] = (acc[...] + dot(mixed, proj[l])).astype(BF)

    def forward(more, i, carry):
        l, c0 = i // n_groups, lax.rem(i, n_groups) * GROUP
        g = i * GROUP

        if more:
            @pl.when(c0 == 0)
            def _():
                begin_forward(l)

            @pl.when(i == 2)
            def _():
                serve()

        wait_group(g)
        fwd_up(l, g, c0, 0, more)
        fwd_up(l, g + 1, c0 + 1, 1, more)
        fwd_down(g, 0, more)
        fwd_up(l, g + 2, c0 + 2, 2, more)
        fwd_down(g + 1, 1, more)
        fwd_down(g + 2, 2, more)

        @pl.when(c0 == n_chunks - GROUP)
        def _():
            end_forward(l)

        return carry

    load_x.wait()
    load_gate[0].wait()
    begin_forward(0)
    wait_group(0, 0, 1)
    fwd_up(0, jnp.int32(0), 0, 0, True)
    fwd_down(jnp.int32(0), 0, True)
    wait_group(0, 1, GROUP - 1)
    for k in range(1, GROUP):
        fwd_up(0, jnp.int32(k), k, k, True)
    for k in range(1, GROUP):
        fwd_down(jnp.int32(k), k, True)
    send_ids()
    kept = n_layers * n_groups - RING // GROUP
    lax.fori_loop(1, kept, functools.partial(forward, True), 0)
    lax.fori_loop(kept, n_layers * n_groups, functools.partial(forward, False), 0)
    write_out = pltpu.make_async_copy(xs.at[0], out_hbm, wsem.at[0])
    write_out.start()
    load_cot.wait()
    send_rows(0, gval[0])


    def mixed_grad(l):
        return dot_nt(cots[...], proj[l]).astype(BF)

    def send_grads(l):
        d_mixed = mixed_grad(l).astype(F32)
        send_rows(l, gval[l] * d_mixed)
        return d_mixed

    mixed_out, mixed_in = served.at[0], fetch_in.at[0]

    def to_partner(l):
        return partner_copy(grad_in.at[l], rows_hbm.at[1, l], dsem.at[0, l], dsem.at[1, l])

    def to_hbm(l):
        return pltpu.make_async_copy(grad_in.at[l], rows_hbm.at[0, l], wsem.at[1 + l])

    def mixed_desc():
        return blocks_desc(n_emb, mixed_out, mixed_in, msem.at[0], msem.at[1])

    def hand_over(l):
        blocks_desc(n_emb, grad_out.at[l], grad_in.at[l], gsem.at[0, l], gsem.at[1, l]).wait()
        grad_in[l, me] = grad_out[l, me]
        if l == 0:
            mixed_desc().wait()
            mixed_in[me] = mixed_out[me]
            grad_in[0] = grad_in[0] * mixed_in[...].astype(F32)
        to_partner(l).start()
        to_hbm(l).start()

    def begin_backward(l):
        d_mixed = send_grads(l)
        for q in range(2, n_layers):
            @pl.when(l == q - 1)
            def _():
                hand_over(q)

        d_gate = (gder[l] * (d_mixed * fetched[l].astype(F32))).astype(BF)
        us[...] = dot_nt(d_gate, gate[l]).astype(BF)
        acc[...] = jnp.zeros_like(acc)

    def bwd_down(l, g, c, k):
        w = wdn.at[lax.rem(g, RING)]
        for j in range(n_sub):
            cols = slice(j * 256, (j + 1) * 256)
            dh = dot_nt(cots[...], w[cols, :]).astype(BF).astype(F32)
            hid[k, :, cols] = (gp[lax.rem(l + 1, 2), c, :, cols] * dh).astype(BF)

    def bwd_up(g, k):
        acc[...] += dot_nt(hid[k], wup[lax.rem(g, RING)])

    def end_backward(l):
        d_norm = (acc[...].astype(BF).astype(F32) + us[...].astype(F32)).astype(BF).astype(F32)
        x = xs[l].astype(F32)
        r = inv_rms(x)
        dx = r * d_norm - x * (r * r * r * jnp.mean(x * d_norm, axis=-1, keepdims=True))
        cots[...] = (cots[...].astype(F32) + dx).astype(BF)

    def backward(i, carry):
        l, place = n_layers - 1 - i // n_groups, lax.rem(i, n_groups)
        g = (n_layers * n_groups + i) * GROUP
        c0 = chunk_of(g)

        @pl.when(place == 0)
        def _():
            begin_backward(l)

        @pl.when(i >= RING // GROUP)
        def _():
            wait_group(g)

        bwd_down(l, g, c0, 0)
        bwd_down(l, g + 1, c0 + 1, 1)
        bwd_up(g, 0)

        @pl.when(g + RING < total)
        def _():
            dn_copy(g + RING).start()
            up_copy(g + RING).start()
            dn_copy(g + 1 + RING).start()

        bwd_down(l, g + 2, c0 + 2, 2)
        bwd_up(g + 1, 1)
        bwd_up(g + 2, 2)

        @pl.when(g + RING < total)
        def _():
            up_copy(g + 1 + RING).start()
            dn_copy(g + 2 + RING).start()
            up_copy(g + 2 + RING).start()

        @pl.when(place == n_groups - 1)
        def _():
            end_backward(l)

        return carry

    lax.fori_loop(0, (n_layers - 1) * n_groups, backward, 0)
    mixed_out[...] = dot(st[...], mixed_grad(0)).astype(BF).reshape(mixed_out.shape)
    send_blocks(n_emb, mixed_out, mixed_in, msem.at[0], msem.at[1])
    hand_over(1)
    hand_over(0)
    ids_to_partner.wait()
    write_out.wait()
    for l in reversed(range(n_layers)):
        to_hbm(l).wait()
        to_partner(l).wait()


def step(n_emb, tok_ids, resid, cot, tables, w_up, w_down, w_gate, w_proj, tf):
    t, d = resid.shape
    n_layers, n_rows, e = tables.shape
    f = w_up.shape[2]
    n_slots = n_emb * CAP
    vmem, hbm = pl.BlockSpec(memory_space=pltpu.VMEM), pl.BlockSpec(memory_space=pl.ANY)
    dma = pltpu.SemaphoreType.DMA
    return pl.pallas_call(
        functools.partial(step_kernel, n_layers, n_emb),
        out_shape=(jax.ShapeDtypeStruct((t, d), BF),
                   jax.ShapeDtypeStruct((2, n_layers, n_emb, CAP, e), F32),
                   jax.ShapeDtypeStruct((2, 8, 128), jnp.int32)),
        in_specs=[vmem] + [hbm] * 7,
        out_specs=(hbm, hbm, vmem),
        scratch_shapes=[
            pltpu.VMEM((RING, d, tf), BF),
            pltpu.VMEM((RING, tf, d), BF),
            pltpu.VMEM((n_layers, d, e), BF),
            pltpu.VMEM((n_layers, e, d), BF),
            pltpu.VMEM((2, f // tf, t, tf), F32),
            pltpu.VMEM((t, d), F32),
            pltpu.VMEM((n_layers, t, d), BF),
            pltpu.VMEM((t, d), BF),
            pltpu.VMEM((t, d), BF),
            pltpu.VMEM((GROUP, t, tf), BF),
            pltpu.VMEM((n_layers, t, e), F32),
            pltpu.VMEM((n_layers, t, e), F32),
            pltpu.VMEM((n_layers, t, e), BF),
            pltpu.VMEM((n_layers, n_rows, e), BF),
            pltpu.VMEM((n_slots, t), BF),
            pltpu.VMEM((n_emb, 1, 128), jnp.int32),
            pltpu.VMEM((n_emb, 1, 128), jnp.int32),
            pltpu.VMEM((n_layers, n_emb, CAP, e), BF),
            pltpu.VMEM((n_layers, n_emb, CAP, e), BF),
            pltpu.VMEM((n_layers, n_emb, CAP, e), F32),
            pltpu.VMEM((n_layers, n_emb, CAP, e), F32),
            dma((2, RING)), dma((3 + n_layers,)), dma((n_layers,)), dma((2,)), dma((2,)),
            dma((2, n_layers)), dma((2, n_layers)), dma((2, n_layers)), dma((1 + n_layers,)), dma((2,)),
        ],
        compiler_params=pltpu.CompilerParams(collective_id=0, has_side_effects=True, vmem_limit_bytes=VMEM_LIMIT),
        name="step",
    )(tok_ids.reshape(1, t), resid, cot, tables, w_up, w_down, w_gate, w_proj)


def scatter_kernel(n_layers, n_rows, ids_ref, rows_hbm, x_hbm, out_hbm, x_out, rows, x, *scratch):
    acc, (insem, xsem, sem) = scratch[:n_layers], scratch[n_layers:]
    e = rows.shape[4]
    n_emb = rows.shape[2]
    loads = [pltpu.make_async_copy(rows_hbm.at[h], rows.at[h], insem.at[h]) for h in range(2)]
    x_in = pltpu.make_async_copy(x_hbm, x, xsem.at[0])
    x_back = pltpu.make_async_copy(x, x_out, xsem.at[1])
    for ld in loads + [x_in]:
        ld.start()

    def clear(i, carry):
        for l in range(n_layers):
            acc[l][pl.ds(pl.multiple_of(i * 64, 64), 64), :] = jnp.zeros((64, e), F32)
        return carry

    lax.fori_loop(0, n_rows // 64, clear, 0)
    per_row = min(128 // CAP, n_emb)

    for half in range(2):
        loads[half].wait()
        if half == 1:
            x_in.wait()
            x_back.start()
        for i in range(n_emb // per_row):
            def block(p, carry):
                b = i * per_row + p

                def pairs(k0, k1):
                    for k in range(k0, k1, 2):
                        v, w = ids_ref[half, i, p * CAP + k], ids_ref[half, i, p * CAP + k + 1]
                        same = v == w
                        for l in range(n_layers):
                            first, second = rows[half, l, b, k:k + 1, :], rows[half, l, b, k + 1:k + 2, :]
                            at_v, at_w = acc[l][pl.ds(v, 1), :], acc[l][pl.ds(w, 1), :]
                            acc[l][pl.ds(v, 1), :] = at_v + first
                            acc[l][pl.ds(w, 1), :] = at_w + (second + jnp.where(same, first, 0.0))

                pairs(0, CAP // 2)

                @pl.when(ids_ref[half, i, p * CAP + CAP // 2] < n_rows)
                def _():
                    pairs(CAP // 2, CAP)

                return carry

            lax.fori_loop(0, per_row, block, 0)
    outs = [pltpu.make_async_copy(acc[l].at[pl.ds(0, n_rows)], out_hbm.at[l], sem.at[l]) for l in range(n_layers)]
    for cp in outs:
        cp.start()
    for cp in outs + [x_back]:
        cp.wait()


def scatter(ids, rows, x, n_rows):
    _, n_layers, n_emb, _, e = rows.shape
    hbm = pl.BlockSpec(memory_space=pl.ANY)
    return pl.pallas_call(
        functools.partial(scatter_kernel, n_layers, n_rows),
        out_shape=(jax.ShapeDtypeStruct((n_layers, n_rows, e), F32), jax.ShapeDtypeStruct(x.shape, x.dtype)),
        in_specs=[pl.BlockSpec(memory_space=pltpu.SMEM), hbm, hbm],
        out_specs=(hbm, hbm),
        scratch_shapes=[pltpu.VMEM(rows.shape, F32), pltpu.VMEM(x.shape, x.dtype)]
        + [pltpu.VMEM((n_rows + 8, e), F32)] * n_layers
        + [pltpu.SemaphoreType.DMA((2,)), pltpu.SemaphoreType.DMA((2,)), pltpu.SemaphoreType.DMA((n_layers,))],
        compiler_params=pltpu.CompilerParams(vmem_limit_bytes=VMEM_LIMIT),
        name="scatter",
    )(ids, rows, x)


def solution(mesh):
    n_emb = mesh.shape["emb"]
    tok_spec = P(("dp", "emb"))
    act_spec = P(("dp", "emb"), None)
    table_spec = P(None, "emb", None)
    full_spec = P(None, None, None)

    def device_body(tok_ids, resid_in, cot_out, tables, w_up, w_down, w_gate, w_proj):
        f = w_up.shape[2]
        tf = 768 if f % (9 * 768) == 0 else 256
        resid_out, rows, ids = step(n_emb, tok_ids, resid_in, cot_out, tables, w_up, w_down, w_gate, w_proj, tf)
        d_tables, resid_out = scatter(ids, rows, resid_out, tables.shape[1])
        return resid_out, d_tables

    return jax.shard_map(device_body, mesh=mesh,
                         in_specs=(tok_spec, act_spec, act_spec, table_spec, full_spec, full_spec, full_spec, full_spec),
                         out_specs=(act_spec, table_spec), check_vma=False)
```
